32 devices in a mesh: parts: 2 (over y), tile: 8 (over z, x), cond: 2 (over core).
Axes of the slice: x: 2, y: 2, z: 4, core: 2. Of those that a mesh axis runs over, the one named last changes fastest.
Arguments:
- mask: bfloat16 [16, 256, 256], P(('parts', 'tile')), parts along dimension 0, may hold values from -1 to 1
- kernels: bfloat16 [8, 24, 64, 128], P('cond'), may hold values from -6 to 6
- socs_weight: float32 [8, 24], P('cond'), may hold values from 0.02 to 1
- dose: float32 [8], P('cond'), may hold values from 0.8 to 1.25
- threshold: float32 [8], P('cond'), may hold values from 0.5 to 0.85
Outputs:
- band_max: float32 [16, 256, 256], P(('parts', 'tile'), 'cond'), parts along dimension 0
- band_min: float32 [16, 256, 256], P(('parts', 'tile'), 'cond'), parts along dimension 0
The draws below stay inside these ranges and needn't reach their ends.
There are 2 independent parts, one for each index of `parts`. The reference program is written for one: setup_inputs(seed, part) draws one part's arguments, and reference() takes and returns one part's arrays. A program takes and returns all parts, laid end to end along the dimension named above; an argument that names none is the same for every part. Nothing has to cross between parts.
All inputs are finite; a program needn't handle non-finite values.
Results may differ from the reference program's by a relative error of at most 0.0068.
Values may be sent and summed in bfloat16 or wider, within the bound.
No kernel may reach another device: no remote copies, remote signals or barrier semaphores. Data moves between devices by JAX's collectives and lax.ppermute only.
A program may use at most 64 MiB of HBM per device.

```python
import math
import jax
import jax.numpy as jnp
from jax import lax

CORE = 256
MARGIN = 64
BLUR = 8
BAND = 64
KERN = 24
COND = 8
TILES = 8
N_TILE = 8


def levels(own_key, shape, split, smallest, largest):
    def one(dim, shards_of):
        heights = jax.random.uniform(jax.random.fold_in(jax.random.fold_in(own_key, 6), dim), (shards_of,), jnp.float32, smallest / len(split), largest / len(split))
        return jnp.repeat(jnp.exp(heights), shape[dim] // shards_of).reshape((-1,) + (1,) * (len(shape) - dim - 1))

    factor_of = one(*split[0])
    for cut in split[1:]:
        factor_of = factor_of * one(*cut)
    return factor_of


def normal_values(stream_key, shape, scale, bound, cuts=(), held_as=jnp.bfloat16):
    loudness = levels(stream_key, shape, cuts, -0.22, 0.18) if cuts else 1.0
    array = jax.random.normal(stream_key, shape, jnp.float32) * scale * loudness
    return jnp.minimum(jnp.maximum(array, -bound), bound).astype(held_as)


def setup_inputs(seed: int = 0, part: int = 0) -> dict:
    key_of = jax.random.split(jax.random.key(seed), 6)
    own_keys = jax.random.split(jax.random.fold_in(key_of[5], part), 6)
    mask = jnp.clip(jax.random.uniform(own_keys[0], (TILES, CORE, CORE), jnp.float32, -1.0, 1.0) * levels(own_keys[0], (TILES, CORE, CORE), ((0, 8),), -0.4, 0.0), -1.0, 1.0).astype(jnp.bfloat16)
    kernels = normal_values(key_of[1], (COND, KERN, BAND, 2 * BAND), 1.0, 6.0, ((0, 2),))
    socs_weight = jnp.clip(jnp.exp(math.log(1.0) - 3.912023 * jax.random.uniform(key_of[2], (COND, KERN), jnp.float32) ** levels(key_of[2], (COND, KERN), ((0, 2),), -0.2, 0.2)), 0.02, 1.0)
    dose = jnp.clip(0.8 + 0.45 * jax.random.uniform(key_of[3], (COND,), jnp.float32) ** levels(key_of[3], (COND,), ((0, 2),), -0.2, 0.2), 0.8, 1.25)
    threshold = jnp.clip(0.5 + 0.35000002 * jax.random.uniform(key_of[4], (COND,), jnp.float32) ** levels(key_of[4], (COND,), ((0, 2),), -0.2, 0.2), 0.5, 0.85)
    return dict(mask=mask, kernels=kernels, socs_weight=socs_weight, dose=dose, threshold=threshold)


diffusion = 2.0
steepness = 8.0


def phase_table(first, count, pad_width, band_width):
    pixel_index = jnp.arange(count, dtype=jnp.int32) + first
    freq_index = (jnp.arange(band_width, dtype=jnp.int32) - band_width // 2) % pad_width
    turn_count = (pixel_index[:, None] * freq_index[None, :]) % pad_width
    angle_grid = turn_count.astype(jnp.float32) * (2.0 * math.pi / pad_width)
    return jnp.cos(angle_grid).astype(jnp.bfloat16), jnp.sin(angle_grid).astype(jnp.bfloat16)


def blur_table(core):
    offset_grid = jnp.arange(core + 2 * BLUR, dtype=jnp.int32)[None, :] - jnp.arange(core, dtype=jnp.int32)[:, None] - BLUR
    distance = offset_grid.astype(jnp.float32)
    taps_grid = jnp.exp(-distance * distance / (2.0 * diffusion * diffusion))
    taps_grid = jnp.where(jnp.abs(offset_grid) <= BLUR, taps_grid, jnp.zeros_like(taps_grid))
    reach_grid = jnp.arange(-BLUR, BLUR + 1, dtype=jnp.int32).astype(jnp.float32)
    total_taps = jnp.sum(jnp.exp(-reach_grid * reach_grid / (2.0 * diffusion * diffusion)))
    return taps_grid / total_taps


def make_tables(core, band_width):
    pad_width = core + 2 * MARGIN
    cos_in, sin_in = phase_table(0, pad_width, pad_width, band_width)
    cos_out, sin_out = phase_table(MARGIN - BLUR, core + 2 * BLUR, pad_width, band_width)
    return cos_in, sin_in, cos_out, sin_out, blur_table(core)


def expose(window, kernel_set, weights, dose_one, threshold_one, tables):
    cos_in, sin_in, cos_out, sin_out, blur_rows = tables
    pad_width = window.shape[0]
    band_width = cos_in.shape[1]
    hp = lax.Precision.HIGHEST
    part_real = jnp.dot(cos_in.T, window, preferred_element_type=jnp.float32).astype(jnp.bfloat16)
    part_imag = (-jnp.dot(sin_in.T, window, preferred_element_type=jnp.float32)).astype(jnp.bfloat16)
    spec_real = (jnp.dot(part_real, cos_in, preferred_element_type=jnp.float32) + jnp.dot(part_imag, sin_in, preferred_element_type=jnp.float32)) / pad_width
    spec_imag = (jnp.dot(part_imag, cos_in, preferred_element_type=jnp.float32) - jnp.dot(part_real, sin_in, preferred_element_type=jnp.float32)) / pad_width
    group_size = min(8, kernel_set.shape[0])
    kernel_groups = kernel_set.reshape(-1, group_size, band_width, 2 * band_width)
    weight_groups = weights.reshape(-1, group_size)
    cos_wide = cos_out.astype(jnp.float32)
    sin_wide = sin_out.astype(jnp.float32)

    def group_power(packed):
        kernel_part, weight_part = packed
        kern_real = kernel_part[:, :, :band_width].astype(jnp.float32)
        kern_imag = kernel_part[:, :, band_width:].astype(jnp.float32)
        prod_real = (spec_real * kern_real - spec_imag * kern_imag).astype(jnp.bfloat16).astype(jnp.float32)
        prod_imag = (spec_real * kern_imag + spec_imag * kern_real).astype(jnp.bfloat16).astype(jnp.float32)
        half_real = (jnp.einsum('nfg,yg->nfy', prod_real, cos_wide, precision=hp) - jnp.einsum('nfg,yg->nfy', prod_imag, sin_wide, precision=hp)).astype(jnp.bfloat16).astype(jnp.float32)
        half_imag = (jnp.einsum('nfg,yg->nfy', prod_real, sin_wide, precision=hp) + jnp.einsum('nfg,yg->nfy', prod_imag, cos_wide, precision=hp)).astype(jnp.bfloat16).astype(jnp.float32)
        field_real = (jnp.einsum('xf,nfy->nxy', cos_wide, half_real, precision=hp) - jnp.einsum('xf,nfy->nxy', sin_wide, half_imag, precision=hp)) / band_width
        field_imag = (jnp.einsum('xf,nfy->nxy', cos_wide, half_imag, precision=hp) + jnp.einsum('xf,nfy->nxy', sin_wide, half_real, precision=hp)) / band_width
        power = field_real * field_real + field_imag * field_imag
        return jnp.tensordot(weight_part, power, axes=1, precision=hp)

    intensity = jnp.sum(lax.map(group_power, (kernel_groups, weight_groups)), axis=0) / jnp.sum(weights)
    blurred = jnp.dot(jnp.dot(blur_rows, intensity, precision=hp), blur_rows.T, precision=hp)
    return jax.nn.sigmoid(steepness * (dose_one * blurred - threshold_one))


def reference(mask, kernels, socs_weight, dose, threshold):
    count = mask.shape[0]
    core = mask.shape[1]
    columns = min(8, N_TILE // 2)
    grid_rows = count // columns
    rotate = columns // 2
    holder = (jnp.arange(count, dtype=jnp.int32) - rotate) % count
    placed = mask[holder]
    region_plane = placed.reshape(grid_rows, columns, core, core).transpose(0, 2, 1, 3).reshape(grid_rows * core, columns * core)
    padded = jnp.pad(region_plane, MARGIN)
    tables = make_tables(core, kernels.shape[2])
    pad_width = core + 2 * MARGIN

    def one_tile(index):
        position = (index + rotate) % count
        top_row = ((position // columns) * core).astype(jnp.int32)
        left_col = ((position % columns) * core).astype(jnp.int32)
        window = lax.dynamic_slice(padded, (top_row, left_col), (pad_width, pad_width))

        def one_condition(packed):
            kernel_set, weights, dose_one, threshold_one = packed
            return expose(window, kernel_set, weights, dose_one, threshold_one, tables)

        resist = lax.map(one_condition, (kernels, socs_weight, dose, threshold))
        return jnp.max(resist, axis=0), jnp.min(resist, axis=0)

    highest, lowest = lax.map(one_tile, jnp.arange(count, dtype=jnp.int32))
    return highest, lowest
```

```python
import math

import jax
import jax.numpy as jnp
import numpy as np
from jax import lax
from jax.experimental import pallas as pl
from jax.experimental.pallas import tpu as pltpu
from jax.sharding import PartitionSpec as P

MARGIN = 64
BLUR = 8

diffusion = 2.0
steepness = 8.0


def phases(pixels, freqs, period):
    angle = 2.0 * np.pi * ((pixels[:, None] * freqs[None, :]) % period) / period
    return np.cos(angle), np.sin(angle)


def make_tables(core, band):
    pad = core + 2 * MARGIN
    freqs = np.arange(band) - band // 2
    cos_in, sin_in = phases(np.arange(pad), freqs, pad)
    row_all = np.concatenate([cos_in, -sin_in], axis=1).T
    row_core = row_all[:, MARGIN : MARGIN + core]
    row_side = np.stack([row_all[:, :MARGIN], row_all[:, MARGIN + core :]])
    order = np.concatenate(
        [np.arange(MARGIN, MARGIN + core), np.arange(MARGIN + core, pad), np.arange(MARGIN)]
    )
    col_real = np.concatenate([cos_in, -sin_in], axis=1)[order]
    col_imag = np.concatenate([sin_in, cos_in], axis=1)[order]
    grid = 2 * band
    cos_g, sin_g = phases(np.arange(grid), freqs, grid)
    half_table = np.concatenate(
        [np.concatenate([cos_g.T, sin_g.T], axis=1), np.concatenate([-sin_g.T, cos_g.T], axis=1)],
        axis=0,
    )
    field_table = np.concatenate(
        [np.concatenate([cos_g, -sin_g], axis=1), np.concatenate([sin_g, cos_g], axis=1)], axis=0
    )
    pixel = np.arange(core + 2 * BLUR) + MARGIN - BLUR
    sample = np.arange(grid) * (pad / grid)
    degrees = np.arange(1, grid // 2)
    gap = pixel[:, None] - sample[None, :]
    interp = (
        1.0 + 2.0 * np.cos(2.0 * np.pi * gap[:, :, None] * degrees / pad).sum(axis=-1)
    ) / grid
    offset = np.arange(core + 2 * BLUR)[None, :] - np.arange(core)[:, None] - BLUR
    taps = np.where(
        np.abs(offset) <= BLUR, np.exp(-(offset**2) / (2.0 * diffusion * diffusion)), 0.0
    )
    reach = np.arange(-BLUR, BLUR + 1)
    taps = taps / np.exp(-(reach**2) / (2.0 * diffusion * diffusion)).sum()
    spread = taps @ interp
    return row_core, row_side, col_real, col_imag, half_table, field_table, spread


def split(value):
    high = value.astype(jnp.bfloat16)
    low = (value - high.astype(jnp.float32)).astype(jnp.bfloat16)
    return high, low


def dot(a, b):
    return jnp.dot(a, b, preferred_element_type=jnp.float32)


def imaging(
    scal_ref,
    place_ref,
    tile_ref,
    left_ref,
    right_ref,
    *rest,
    sides,
    pad,
):
    upright_refs = rest[: len(sides)]
    (
        kern_ref,
        row_core_ref,
        row_side_ref,
        col_real_ref,
        col_imag_ref,
        half_ref,
        field_ref,
        spread_ref,
        across_ref,
        keep_ref,
        send_ref,
        halves_ref,
        coarse_ref,
    ) = rest[len(sides) :]
    conds, kerns, band, _ = kern_ref.shape
    grid = 2 * band
    core = tile_ref.shape[0]
    lane = lax.broadcasted_iota(jnp.int32, (core, 2 * MARGIN), 1)
    right_ok = place_ref[0] > 0
    left_ok = place_ref[1] > 0
    zero = jnp.zeros((core, 2 * MARGIN), jnp.float32)
    ring = jnp.where(
        lane < MARGIN,
        jnp.where(right_ok, right_ref[...].astype(jnp.float32), zero),
        jnp.where(left_ok, left_ref[...].astype(jnp.float32), zero),
    ).astype(jnp.bfloat16)
    part_core = dot(row_core_ref[...], tile_ref[...])
    part_ring = dot(row_core_ref[...], ring)
    lane = lane[:MARGIN]
    edge_ok = jnp.where(lane < MARGIN, place_ref[0], place_ref[1]) > 0
    for n, side in enumerate(sides):
        there = place_ref[2 + n] > 0
        table = row_side_ref[place_ref[4]] if side is None else row_side_ref[side]
        strip = upright_refs[n][...].astype(jnp.float32)
        strip = jnp.where(there, strip, jnp.zeros_like(strip))
        edge = jnp.where(edge_ok, strip[:, core:], jnp.zeros_like(strip[:, core:]))
        part_core = part_core + dot(table, strip[:, :core].astype(jnp.bfloat16))
        part_ring = part_ring + dot(table, edge.astype(jnp.bfloat16))
    part = jnp.concatenate([part_core, part_ring], axis=1).astype(jnp.bfloat16)
    spec = dot(part[:band], col_real_ref[...]) + dot(part[band:], col_imag_ref[...])
    spec = spec * (1.0 / pad)
    swapped = pltpu.roll(spec, band, 1)
    first = lax.broadcasted_iota(jnp.int32, spec.shape, 1) < band
    spec_same = jnp.where(first, spec, swapped)
    spec_cross = jnp.where(first, -swapped, spec)

    def condition(c, carry):
        prods = []
        for k in range(kerns):
            kern = kern_ref[c, k].astype(jnp.float32)
            prod = kern * spec_same + pltpu.roll(kern, band, 1) * spec_cross
            prods.append(prod.astype(jnp.bfloat16))
        halves_ref[...] = dot(jnp.concatenate(prods, axis=0), half_ref[...]).astype(jnp.bfloat16)
        total = jnp.zeros((grid, grid), jnp.float32)
        for k in range(0, kerns, 2):
            a = halves_ref[k * band : (k + 1) * band]
            b = halves_ref[(k + 1) * band : (k + 2) * band]
            both = jnp.concatenate(
                [
                    jnp.concatenate([a[:, :grid], b[:, :grid]], axis=1),
                    jnp.concatenate([a[:, grid:], b[:, grid:]], axis=1),
                ],
                axis=0,
            )
            field = dot(field_ref[...], both)
            power = field[:grid] * field[:grid] + field[grid:] * field[grid:]
            total = total + scal_ref[c, k] * power[:, :grid] + scal_ref[c, k + 1] * power[:, grid:]
        coarse_ref[c] = total
        return carry

    lax.fori_loop(0, conds, condition, 0)
    coarse = coarse_ref[...].reshape(conds * grid, grid)
    high, low = split(coarse)
    across = (
        dot(high, across_ref[0])
        + dot(low, across_ref[0])
        + dot(high, across_ref[1])
    )
    high, low = split(across)
    own = place_ref[5]
    share = core // 2
    for turn in range(2):
        part_of = 1 - own if turn == 0 else own
        rows = pl.ds(pl.multiple_of(part_of * share, share), share)
        most = None
        for c in range(conds):
            h = high[c * grid : (c + 1) * grid]
            l = low[c * grid : (c + 1) * grid]
            blurred = dot(spread_ref[0, rows], h)
            blurred = blurred + dot(spread_ref[0, rows], l) + dot(spread_ref[1, rows], h)
            level = scal_ref[c, kerns] * blurred - scal_ref[c, kerns + 1]
            most = level if most is None else jnp.maximum(most, level)
            least = level if c == 0 else jnp.minimum(least, level)
        if turn == 0:
            send_ref[0] = jax.nn.sigmoid(most).astype(jnp.bfloat16)
            send_ref[1] = jax.nn.sigmoid(least).astype(jnp.bfloat16)
        else:
            keep_ref[0] = jax.nn.sigmoid(most)
            keep_ref[1] = jax.nn.sigmoid(least)


def two_parts(table):
    high = np.asarray(table, np.float32).astype(jnp.bfloat16)
    low = (table - high.astype(np.float64)).astype(jnp.bfloat16)
    return np.stack([high, low])


def shifted(block, axis, distance):
    count = lax.axis_size(axis)
    return lax.ppermute(block, axis, [((i - distance) % count, i) for i in range(count)])


def on_device(mask, kernels, socs_weight, dose, threshold):
    tile = mask[0]
    core = tile.shape[0]
    conds, kerns, band, _ = kernels.shape
    pad = core + 2 * MARGIN
    grid = 2 * band
    count = lax.axis_size("tile")
    columns = min(8, count // 2)
    grid_rows = count // columns
    position = (lax.axis_index("tile") + columns // 2) % count
    column = position % columns
    row = position // columns

    left = shifted(tile[:, -2 * MARGIN :], "tile", 1)
    right = shifted(tile[:, : 2 * MARGIN], "tile", -1)

    def wide(rows):
        lane = lax.broadcasted_iota(jnp.int32, (MARGIN, 2 * MARGIN), 1)
        edge = jnp.where(lane < MARGIN, right[rows], left[rows])
        return jnp.concatenate([tile[rows], edge], axis=1)

    top, bottom = slice(0, MARGIN), slice(core - MARGIN, core)
    if grid_rows == 2:
        sides = (None,)
        strips = [shifted(jnp.where(row == 0, wide(bottom), wide(top)), "tile", columns)]
        there = [1, 1]
    else:
        sides = (0, 1)
        strips = [
            shifted(wide(bottom), "tile", columns),
            shifted(wide(top), "tile", -columns),
        ]
        there = [row > 0, row < grid_rows - 1]
    place = jnp.stack(
        [
            jnp.asarray(v, jnp.int32)
            for v in (column < columns - 1, column > 0, *there, row == 0, lax.axis_index("cond"))
        ]
    )
    norm = socs_weight / (jnp.sum(socs_weight, axis=1, keepdims=True) * (band * band))
    scal = jnp.concatenate(
        [norm, steepness * dose[:, None], steepness * threshold[:, None]], axis=1
    )
    row_core, row_side, col_real, col_imag, half_t, field_t, spread = make_tables(core, band)
    bf = lambda t: np.asarray(t).astype(jnp.bfloat16)
    consts = (
        bf(row_core),
        bf(row_side),
        bf(col_real),
        bf(col_imag),
        bf(half_t),
        bf(field_t),
        two_parts(spread),
        two_parts(spread.T),
    )
    smem = pl.BlockSpec(memory_space=pltpu.SMEM)
    vmem = pl.BlockSpec(memory_space=pltpu.VMEM)
    share = core // lax.axis_size("cond")
    keep, send = pl.pallas_call(
        lambda *refs: imaging(*refs, sides=sides, pad=pad),
        out_shape=(
            jax.ShapeDtypeStruct((2, share, core), jnp.float32),
            jax.ShapeDtypeStruct((2, share, core), jnp.bfloat16),
        ),
        in_specs=[smem, smem] + [vmem] * (4 + len(strips) + len(consts)),
        out_specs=(vmem, vmem),
        scratch_shapes=[
            pltpu.VMEM((kerns * band, 2 * grid), jnp.bfloat16),
            pltpu.VMEM((conds, grid, grid), jnp.float32),
        ],
        name="imaging",
    )(scal, place, tile, left, right, *strips, kernels, *[jnp.asarray(t) for t in consts])
    other = lax.ppermute(send, "cond", [(0, 1), (1, 0)]).astype(jnp.float32)
    return (jnp.maximum(keep[0], other[0])[None], jnp.minimum(keep[1], other[1])[None])


def solution(mesh):
    return jax.shard_map(
        on_device,
        mesh=mesh,
        in_specs=(
            P(("parts", "tile"), None, None),
            P("cond", None, None, None),
            P("cond", None),
            P("cond"),
            P("cond"),
        ),
        out_specs=(P(("parts", "tile"), "cond", None), P(("parts", "tile"), "cond", None)),
        check_vma=False,
    )
```

```python
import math

import jax
import jax.numpy as jnp
import numpy as np
from jax import lax
from jax.experimental import pallas as pl
from jax.experimental.pallas import tpu as pltpu
from jax.sharding import PartitionSpec as P

MARGIN = 64
BLUR = 8

diffusion = 2.0
steepness = 8.0


def phases(pixels, freqs, period):
    angle = 2.0 * np.pi * ((pixels[:, None] * freqs[None, :]) % period) / period
    return np.cos(angle), np.sin(angle)


def make_tables(core, band):
    pad = core + 2 * MARGIN
    freqs = np.arange(band) - band // 2
    cos_in, sin_in = phases(np.arange(pad), freqs, pad)
    row_all = np.concatenate([cos_in, -sin_in], axis=1).T
    row_core = row_all[:, MARGIN : MARGIN + core]
    row_side = np.stack([row_all[:, :MARGIN], row_all[:, MARGIN + core :]])
    order = np.concatenate(
        [np.arange(MARGIN, MARGIN + core), np.arange(MARGIN + core, pad), np.arange(MARGIN)]
    )
    col_real = np.concatenate([cos_in, -sin_in], axis=1)[order]
    col_imag = np.concatenate([sin_in, cos_in], axis=1)[order]
    grid = 2 * band
    cos_g, sin_g = phases(np.arange(grid), freqs, grid)
    half_table = np.concatenate(
        [np.concatenate([cos_g.T, sin_g.T], axis=1), np.concatenate([-sin_g.T, cos_g.T], axis=1)],
        axis=0,
    )
    field_table = np.concatenate(
        [np.concatenate([cos_g, -sin_g], axis=1), np.concatenate([sin_g, cos_g], axis=1)], axis=0
    )
    pixel = np.arange(core + 2 * BLUR) + MARGIN - BLUR
    sample = np.arange(grid) * (pad / grid)
    degrees = np.arange(1, grid // 2)
    gap = pixel[:, None] - sample[None, :]
    interp = (
        1.0 + 2.0 * np.cos(2.0 * np.pi * gap[:, :, None] * degrees / pad).sum(axis=-1)
    ) / grid
    offset = np.arange(core + 2 * BLUR)[None, :] - np.arange(core)[:, None] - BLUR
    taps = np.where(
        np.abs(offset) <= BLUR, np.exp(-(offset**2) / (2.0 * diffusion * diffusion)), 0.0
    )
    reach = np.arange(-BLUR, BLUR + 1)
    taps = taps / np.exp(-(reach**2) / (2.0 * diffusion * diffusion)).sum()
    spread = taps @ interp
    return row_core, row_side, col_real, col_imag, half_table, field_table, spread


def split(value):
    high = value.astype(jnp.bfloat16)
    low = (value - high.astype(jnp.float32)).astype(jnp.bfloat16)
    return high, low


def dot(a, b):
    return jnp.dot(a, b, preferred_element_type=jnp.float32)


def placement():
    count = lax.axis_size("tile")
    columns = min(8, count // 2)
    grid_rows = count // columns
    position = (lax.axis_index("tile") + columns // 2) % count
    column = position % columns
    row = position // columns
    return dict(
        columns=columns,
        grid_rows=grid_rows,
        right=column < columns - 1,
        left=column > 0,
        above=row > 0,
        below=row < grid_rows - 1,
        top=row == 0,
        half=lax.axis_index("cond"),
    )


def dma_all(pairs, sems):
    return [pltpu.make_async_copy(src, dst, sems.at[n]) for n, (src, dst) in enumerate(pairs)]


def staging(tile_ref, *refs):
    count = (len(refs) - 3) // 2
    sources, targets = refs[:count], refs[count : 2 * count]
    part_ref, tile_v, sems = refs[2 * count :]
    copies = dma_all([(tile_ref, tile_v)] + list(zip(sources, targets)), sems)
    for copy in copies:
        copy.start()
    copies[0].wait()
    copies[1].wait()
    part_ref[...] = dot(targets[0][...], tile_v[...])
    for copy in copies[2:]:
        copy.wait()


def imaging(weight_hbm, dose_hbm, threshold_hbm, part_ref, left_ref, right_ref, *rest, sides, pad):
    place = placement()
    upright_refs = rest[: len(sides)]
    (
        row_core_ref,
        row_side_ref,
        col_real_ref,
        col_imag_ref,
        half_ref,
        field_ref,
        spread_ref,
        across_ref,
        kern_ref,
        send_ref,
        level_ref,
        gain_ref,
        halves_ref,
        coarse_ref,
        weight_ref,
        dose_ref,
        threshold_ref,
        sems,
    ) = rest[len(sides) :]
    copies = dma_all(
        [(weight_hbm, weight_ref), (dose_hbm, dose_ref), (threshold_hbm, threshold_ref)], sems
    )
    for copy in copies:
        copy.start()
    conds, kerns, band, _ = kern_ref.shape
    grid = 2 * band
    core = part_ref.shape[1]
    lane = lax.broadcasted_iota(jnp.int32, (core, 2 * MARGIN), 1)
    right_ok, left_ok = place["right"], place["left"]
    zero = jnp.zeros((core, 2 * MARGIN), jnp.float32)
    ring = jnp.where(
        lane < MARGIN,
        jnp.where(right_ok, right_ref[...].astype(jnp.float32), zero),
        jnp.where(left_ok, left_ref[...].astype(jnp.float32), zero),
    ).astype(jnp.bfloat16)
    part_core = part_ref[...]
    part_ring = dot(row_core_ref[...], ring)
    lane = lane[:MARGIN]
    for n, side in enumerate(sides):
        strip = upright_refs[n][...].astype(jnp.float32)
        if side is None:
            table = row_side_ref[place["top"].astype(jnp.int32)]
        else:
            table = row_side_ref[side]
            there = place["below"] if side else place["above"]
            strip = jnp.where(there, strip, jnp.zeros_like(strip))
        none = jnp.zeros_like(strip[:, core:])
        edge = jnp.where(
            lane < MARGIN,
            jnp.where(right_ok, strip[:, core:], none),
            jnp.where(left_ok, strip[:, core:], none),
        )
        part_core = part_core + dot(table, strip[:, :core].astype(jnp.bfloat16))
        part_ring = part_ring + dot(table, edge.astype(jnp.bfloat16))
    part = jnp.concatenate([part_core, part_ring], axis=1).astype(jnp.bfloat16)
    spec = dot(part[:band], col_real_ref[...]) + dot(part[band:], col_imag_ref[...])
    spec = spec * (1.0 / pad)
    swapped = pltpu.roll(spec, band, 1)
    first = lax.broadcasted_iota(jnp.int32, spec.shape, 1) < band
    spec_same = jnp.where(first, spec, swapped)
    spec_cross = jnp.where(first, -swapped, spec)
    for copy in copies:
        copy.wait()

    def condition(c, carry):
        prods = []
        for k in range(kerns):
            kern = kern_ref[c, k].astype(jnp.float32)
            prod = kern * spec_same + pltpu.roll(kern, band, 1) * spec_cross
            prods.append(prod.astype(jnp.bfloat16))
        halves_ref[...] = dot(jnp.concatenate(prods, axis=0), half_ref[...]).astype(jnp.bfloat16)
        total = jnp.zeros((grid, grid), jnp.float32)
        for k in range(0, kerns, 2):
            a = halves_ref[k * band : (k + 1) * band]
            b = halves_ref[(k + 1) * band : (k + 2) * band]
            both = jnp.concatenate(
                [
                    jnp.concatenate([a[:, :grid], b[:, :grid]], axis=1),
                    jnp.concatenate([a[:, grid:], b[:, grid:]], axis=1),
                ],
                axis=0,
            )
            field = dot(field_ref[...], both)
            power = field[:grid] * field[:grid] + field[grid:] * field[grid:]
            total = (
                total + weight_ref[c, k] * power[:, :grid] + weight_ref[c, k + 1] * power[:, grid:]
            )
        coarse_ref[c] = total
        return carry

    lax.fori_loop(0, conds, condition, 0)
    high, low = split(coarse_ref[...].reshape(conds * grid, grid))
    across = dot(high, across_ref[0]) + dot(low, across_ref[0]) + dot(high, across_ref[1])
    level_ref[0], level_ref[1] = split(across)
    for c in range(conds):
        mass = weight_ref[c, 0]
        for k in range(1, kerns):
            mass = mass + weight_ref[c, k]
        gain_ref[0, c] = steepness * dose_ref[c] / jnp.full((8, core), mass * float(band * band))
        gain_ref[1, c] = jnp.full((8, core), steepness * threshold_ref[c])
    most, least = band_of(1 - place["half"], level_ref, gain_ref, spread_ref)
    send_ref[0] = most.astype(jnp.bfloat16)
    send_ref[1] = least.astype(jnp.bfloat16)


def band_of(part_of, level_ref, gain_ref, spread_ref):
    conds = gain_ref.shape[1]
    core = spread_ref.shape[1]
    grid = level_ref.shape[1] // conds
    share = core // 2
    rows = pl.ds(pl.multiple_of(part_of * share, share), share)
    for c in range(conds):
        h = level_ref[0, c * grid : (c + 1) * grid]
        l = level_ref[1, c * grid : (c + 1) * grid]
        blurred = dot(spread_ref[0, rows], h)
        blurred = blurred + dot(spread_ref[0, rows], l) + dot(spread_ref[1, rows], h)
        level = gain_ref[0, c, :1] * blurred - gain_ref[1, c, :1]
        most = level if c == 0 else jnp.maximum(most, level)
        least = level if c == 0 else jnp.minimum(least, level)
    return jax.nn.sigmoid(most), jax.nn.sigmoid(least)


def own_share(level_ref, gain_ref, spread_ref, keep_ref):
    keep_ref[0], keep_ref[1] = band_of(lax.axis_index("cond"), level_ref, gain_ref, spread_ref)


def two_parts(table):
    high = np.asarray(table, np.float32).astype(jnp.bfloat16)
    low = (table - high.astype(np.float64)).astype(jnp.bfloat16)
    return np.stack([high, low])


def in_hbm(value):
    return pltpu.with_memory_space_constraint(value, pltpu.HBM)


def shifted(block, axis, distance):
    count = lax.axis_size(axis)
    return lax.ppermute(block, axis, [((i - distance) % count, i) for i in range(count)])


def on_device(mask, kernels, socs_weight, dose, threshold):
    tile = mask[0]
    core = tile.shape[0]
    conds, kerns, band, _ = kernels.shape
    pad = core + 2 * MARGIN
    grid = 2 * band
    place = placement()
    columns, grid_rows = place["columns"], place["grid_rows"]

    left = shifted(tile[:, -2 * MARGIN :], "tile", 1)
    right = shifted(tile[:, : 2 * MARGIN], "tile", -1)

    def wide(rows):
        lane = lax.broadcasted_iota(jnp.int32, (MARGIN, 2 * MARGIN), 1)
        edge = jnp.where(lane < MARGIN, right[rows], left[rows])
        return jnp.concatenate([tile[rows], edge], axis=1)

    top, bottom = slice(0, MARGIN), slice(core - MARGIN, core)
    if grid_rows == 2:
        sides = (None,)
        strips = [shifted(jnp.where(place["top"], wide(bottom), wide(top)), "tile", columns)]
    else:
        sides = (0, 1)
        strips = [
            shifted(wide(bottom), "tile", columns),
            shifted(wide(top), "tile", -columns),
        ]
    row_core, row_side, col_real, col_imag, half_t, field_t, spread = make_tables(core, band)
    bf = lambda t: np.asarray(t).astype(jnp.bfloat16)
    consts = (
        bf(row_core),
        bf(row_side),
        bf(col_real),
        bf(col_imag),
        bf(half_t),
        bf(field_t),
        two_parts(spread),
        two_parts(spread.T),
    )
    consts = [jnp.asarray(t) for t in consts] + [kernels]
    vmem = pl.BlockSpec(memory_space=pltpu.VMEM)
    hbm = pl.BlockSpec(memory_space=pltpu.HBM)
    share = core // lax.axis_size("cond")
    params = pltpu.CompilerParams(vmem_limit_bytes=16 * 2**20)
    *staged, part = pl.pallas_call(
        staging,
        out_shape=[jax.ShapeDtypeStruct(t.shape, t.dtype) for t in consts]
        + [jax.ShapeDtypeStruct((2 * band, core), jnp.float32)],
        in_specs=[hbm] * (1 + len(consts)),
        out_specs=[vmem] * (1 + len(consts)),
        scratch_shapes=[
            pltpu.VMEM((core, core), jnp.bfloat16),
            pltpu.SemaphoreType.DMA((1 + len(consts),)),
        ],
        compiler_params=params,
        name="staging",
    )(in_hbm(tile), *map(in_hbm, consts))
    send, level, gain = pl.pallas_call(
        lambda *refs: imaging(*refs, sides=sides, pad=pad),
        out_shape=(
            jax.ShapeDtypeStruct((2, share, core), jnp.bfloat16),
            jax.ShapeDtypeStruct((2, conds * grid, core), jnp.bfloat16),
            jax.ShapeDtypeStruct((2, conds, 8, core), jnp.float32),
        ),
        in_specs=[hbm] * 3 + [vmem] * (3 + len(strips) + len(staged)),
        out_specs=(vmem, vmem, vmem),
        scratch_shapes=[
            pltpu.VMEM((kerns * band, 2 * grid), jnp.bfloat16),
            pltpu.VMEM((conds, grid, grid), jnp.float32),
            pltpu.SMEM(socs_weight.shape, jnp.float32),
            pltpu.SMEM(dose.shape, jnp.float32),
            pltpu.SMEM(threshold.shape, jnp.float32),
            pltpu.SemaphoreType.DMA((3,)),
        ],
        compiler_params=params,
        name="imaging",
    )(in_hbm(socs_weight), in_hbm(dose), in_hbm(threshold), part, left, right, *strips, *staged)
    other = lax.ppermute(send, "cond", [(0, 1), (1, 0)])
    keep = pl.pallas_call(
        own_share,
        out_shape=jax.ShapeDtypeStruct((2, share, core), jnp.float32),
        in_specs=[vmem] * 3,
        out_specs=vmem,
        compiler_params=params,
        name="own_share",
    )(level, gain, staged[6])
    other = other.astype(jnp.float32)
    return (jnp.maximum(keep[0], other[0])[None], jnp.minimum(keep[1], other[1])[None])


def solution(mesh):
    return jax.shard_map(
        on_device,
        mesh=mesh,
        in_specs=(
            P(("parts", "tile"), None, None),
            P("cond", None, None, None),
            P("cond", None),
            P("cond"),
            P("cond"),
        ),
        out_specs=(P(("parts", "tile"), "cond", None), P(("parts", "tile"), "cond", None)),
        check_vma=False,
    )
```

```python
import math

import jax
import jax.numpy as jnp
import numpy as np
from jax import lax
from jax.experimental import pallas as pl
from jax.experimental.pallas import tpu as pltpu
from jax.sharding import PartitionSpec as P

MARGIN = 64
BLUR = 8

diffusion = 2.0
steepness = 8.0


def phases(pixels, freqs, period):
    angle = 2.0 * np.pi * ((pixels[:, None] * freqs[None, :]) % period) / period
    return np.cos(angle), np.sin(angle)


def make_tables(core, band):
    pad = core + 2 * MARGIN
    freqs = np.arange(band) - band // 2
    cos_in, sin_in = phases(np.arange(pad), freqs, pad)
    row_all = np.concatenate([cos_in, -sin_in], axis=1).T
    row_core = row_all[:, MARGIN : MARGIN + core]
    row_side = np.stack([row_all[:, :MARGIN], row_all[:, MARGIN + core :]])
    table = np.stack(
        [np.concatenate([cos_in, -sin_in], axis=1), np.concatenate([sin_in, cos_in], axis=1)]
    )
    none = np.zeros((2, MARGIN, 2 * band))
    half = core // 2
    middle = MARGIN + half
    columns = np.stack(
        [
            np.concatenate([table[:, MARGIN:middle], none, table[:, :MARGIN]], axis=1),
            np.concatenate([table[:, middle : middle + half], table[:, -MARGIN:], none], axis=1),
        ]
    )
    grid = 2 * band
    cos_g, sin_g = phases(np.arange(grid), freqs, grid)
    half_table = np.concatenate(
        [np.concatenate([cos_g.T, sin_g.T], axis=1), np.concatenate([-sin_g.T, cos_g.T], axis=1)],
        axis=0,
    )
    field_table = np.concatenate(
        [np.concatenate([cos_g, -sin_g], axis=1), np.concatenate([sin_g, cos_g], axis=1)], axis=0
    )
    pixel = np.arange(core + 2 * BLUR) + MARGIN - BLUR
    sample = np.arange(grid) * (pad / grid)
    degrees = np.arange(1, grid // 2)
    gap = pixel[:, None] - sample[None, :]
    interp = (
        1.0 + 2.0 * np.cos(2.0 * np.pi * gap[:, :, None] * degrees / pad).sum(axis=-1)
    ) / grid
    offset = np.arange(core + 2 * BLUR)[None, :] - np.arange(core)[:, None] - BLUR
    taps = np.where(
        np.abs(offset) <= BLUR, np.exp(-(offset**2) / (2.0 * diffusion * diffusion)), 0.0
    )
    reach = np.arange(-BLUR, BLUR + 1)
    taps = taps / np.exp(-(reach**2) / (2.0 * diffusion * diffusion)).sum()
    spread = taps @ interp
    return row_core, row_side, columns, half_table, field_table, spread


def split(value):
    high = value.astype(jnp.bfloat16)
    low = (value - high.astype(jnp.float32)).astype(jnp.bfloat16)
    return high, low


def dot(a, b):
    return jnp.dot(a, b, preferred_element_type=jnp.float32)


def placement():
    count = lax.axis_size("tile")
    columns = min(8, count // 2)
    grid_rows = count // columns
    position = (lax.axis_index("tile") + columns // 2) % count
    column = position % columns
    row = position // columns
    return dict(
        columns=columns,
        grid_rows=grid_rows,
        right=column < columns - 1,
        left=column > 0,
        above=row > 0,
        below=row < grid_rows - 1,
        top=row == 0,
        half=lax.axis_index("cond"),
    )


def dma_all(pairs, sems):
    return [pltpu.make_async_copy(src, dst, sems.at[n]) for n, (src, dst) in enumerate(pairs)]


def staging(*refs):
    count = (len(refs) - 1) // 2
    own = lax.axis_index("cond")
    sources = [refs[0].at[own], *refs[1:count]]
    copies = dma_all(zip(sources, refs[count : 2 * count]), refs[-1])
    for copy in copies:
        copy.start()
    for copy in copies:
        copy.wait()


def row_analysis(tile_hbm, strip_ref, row_core_ref, part_ref, tile_ref, sem):
    half = tile_ref.shape[1]
    first = pl.multiple_of(lax.axis_index("cond") * half, half)
    copy = pltpu.make_async_copy(tile_hbm.at[:, pl.ds(first, half)], tile_ref, sem)
    copy.start()
    part_ref[:, half:] = dot(row_core_ref[...], strip_ref[...])
    copy.wait()
    part_ref[:, :half] = dot(row_core_ref[...], tile_ref[...])


def spectrum(part_ref, row_side_ref, columns_ref, *rest, sides):
    *upright_refs, spec_ref = rest
    place = placement()
    band = spec_ref.shape[0]
    half = part_ref.shape[1] - 2 * MARGIN
    part = part_ref[...]
    for n, side in enumerate(sides):
        if side is None:
            table = row_side_ref[place["top"].astype(jnp.int32)]
            part = part + dot(table, upright_refs[n][...])
        else:
            there = place["below"] if side else place["above"]
            more = dot(row_side_ref[side], upright_refs[n][...])
            part = part + jnp.where(there, more, jnp.zeros_like(more))
    edge = part[:, half:]
    beside = jnp.where(place["half"] == 0, place["left"], place["right"])
    edge = jnp.where(beside, edge, jnp.zeros_like(edge))
    part = jnp.concatenate([part[:, :half], edge], axis=1).astype(jnp.bfloat16)
    spec_ref[...] = dot(part[:band], columns_ref[0]) + dot(part[band:], columns_ref[1])


def imaging(
    weight_hbm,
    dose_hbm,
    threshold_hbm,
    mine_ref,
    other_ref,
    half_ref,
    field_ref,
    spread_ref,
    across_ref,
    kern_ref,
    send_ref,
    level_ref,
    gain_ref,
    halves_ref,
    coarse_ref,
    weight_ref,
    dose_ref,
    threshold_ref,
    sems,
    *,
    pad,
):
    copies = dma_all(
        [(weight_hbm, weight_ref), (dose_hbm, dose_ref), (threshold_hbm, threshold_ref)], sems
    )
    for copy in copies:
        copy.start()
    conds, kerns, band, _ = kern_ref.shape
    grid = 2 * band
    core = spread_ref.shape[1]
    spec = (mine_ref[...] + other_ref[...]) * (1.0 / pad)
    swapped = pltpu.roll(spec, band, 1)
    first = lax.broadcasted_iota(jnp.int32, spec.shape, 1) < band
    spec_same = jnp.where(first, spec, swapped)
    spec_cross = jnp.where(first, -swapped, spec)
    for copy in copies:
        copy.wait()

    def condition(c, carry):
        prods = []
        for k in range(kerns):
            kern = kern_ref[c, k].astype(jnp.float32)
            prod = kern * spec_same + pltpu.roll(kern, band, 1) * spec_cross
            prods.append(prod.astype(jnp.bfloat16))
        halves_ref[...] = dot(jnp.concatenate(prods, axis=0), half_ref[...]).astype(jnp.bfloat16)
        total = jnp.zeros((grid, grid), jnp.float32)
        for k in range(0, kerns, 2):
            a = halves_ref[k * band : (k + 1) * band]
            b = halves_ref[(k + 1) * band : (k + 2) * band]
            both = jnp.concatenate(
                [
                    jnp.concatenate([a[:, :grid], b[:, :grid]], axis=1),
                    jnp.concatenate([a[:, grid:], b[:, grid:]], axis=1),
                ],
                axis=0,
            )
            field = dot(field_ref[...], both)
            power = field[:grid] * field[:grid] + field[grid:] * field[grid:]
            total = (
                total + weight_ref[c, k] * power[:, :grid] + weight_ref[c, k + 1] * power[:, grid:]
            )
        coarse_ref[c] = total
        return carry

    lax.fori_loop(0, conds, condition, 0)
    high, low = split(coarse_ref[...].reshape(conds * grid, grid))
    across = dot(high, across_ref[0]) + dot(low, across_ref[0]) + dot(high, across_ref[1])
    level_ref[0], level_ref[1] = split(across)
    for c in range(conds):
        mass = weight_ref[c, 0]
        for k in range(1, kerns):
            mass = mass + weight_ref[c, k]
        gain_ref[0, c] = steepness * dose_ref[c] / jnp.full((8, core), mass * float(band * band))
        gain_ref[1, c] = jnp.full((8, core), steepness * threshold_ref[c])
    most, least = band_of(1 - lax.axis_index("cond"), level_ref, gain_ref, spread_ref)
    send_ref[0] = most.astype(jnp.bfloat16)
    send_ref[1] = least.astype(jnp.bfloat16)


def band_of(part_of, level_ref, gain_ref, spread_ref):
    conds = gain_ref.shape[1]
    core = spread_ref.shape[1]
    grid = level_ref.shape[1] // conds
    share = core // 2
    rows = pl.ds(pl.multiple_of(part_of * share, share), share)
    for c in range(conds):
        h = level_ref[0, c * grid : (c + 1) * grid]
        l = level_ref[1, c * grid : (c + 1) * grid]
        blurred = dot(spread_ref[0, rows], h)
        blurred = blurred + dot(spread_ref[0, rows], l) + dot(spread_ref[1, rows], h)
        level = gain_ref[0, c, :1] * blurred - gain_ref[1, c, :1]
        most = level if c == 0 else jnp.maximum(most, level)
        least = level if c == 0 else jnp.minimum(least, level)
    return jax.nn.sigmoid(most), jax.nn.sigmoid(least)


def own_share(level_ref, gain_ref, spread_ref, keep_ref):
    keep_ref[0], keep_ref[1] = band_of(lax.axis_index("cond"), level_ref, gain_ref, spread_ref)


def two_parts(table):
    high = np.asarray(table, np.float32).astype(jnp.bfloat16)
    low = (table - high.astype(np.float64)).astype(jnp.bfloat16)
    return np.stack([high, low])


def in_hbm(value):
    return pltpu.with_memory_space_constraint(value, pltpu.HBM)


def shifted(block, axis, distance):
    count = lax.axis_size(axis)
    return lax.ppermute(block, axis, [((i - distance) % count, i) for i in range(count)])


def on_device(mask, kernels, socs_weight, dose, threshold):
    tile = mask[0]
    core = tile.shape[0]
    conds, kerns, band, _ = kernels.shape
    pad = core + 2 * MARGIN
    grid = 2 * band
    place = placement()
    count = lax.axis_size("tile")
    columns, grid_rows = place["columns"], place["grid_rows"]

    half, wide = core // 2, 2 * MARGIN
    left_core = lax.axis_index("cond") == 0
    others = [((t - 1) % count, t) for t in range(count)]
    route = [(2 * a, 2 * b) for a, b in others] + [(2 * b + 1, 2 * a + 1) for a, b in others]
    strip = lax.ppermute(
        jnp.where(left_core, tile[:, -wide:], tile[:, :wide]), ("tile", "cond"), route
    )
    columns_own = jnp.where(left_core, tile[:, :half], tile[:, half:])
    upper = jnp.concatenate([columns_own[:MARGIN], strip[:MARGIN]], axis=1)
    lower = jnp.concatenate([columns_own[-MARGIN:], strip[-MARGIN:]], axis=1)
    if grid_rows == 2:
        sides = (None,)
        uprights = [shifted(jnp.where(place["top"], lower, upper), "tile", columns)]
    else:
        sides = (0, 1)
        uprights = [shifted(lower, "tile", columns), shifted(upper, "tile", -columns)]
    row_core, row_side, col_table, half_t, field_t, spread = make_tables(core, band)
    bf = lambda t: jnp.asarray(np.asarray(t).astype(jnp.bfloat16))
    fixed = [
        bf(col_table),
        bf(row_core),
        bf(row_side),
        bf(half_t),
        bf(field_t),
        jnp.asarray(two_parts(spread)),
        jnp.asarray(two_parts(spread.T)),
        kernels,
    ]
    vmem = pl.BlockSpec(memory_space=pltpu.VMEM)
    hbm = pl.BlockSpec(memory_space=pltpu.HBM)
    share = core // lax.axis_size("cond")
    params = pltpu.CompilerParams(vmem_limit_bytes=16 * 2**20)
    shapes = [t.shape for t in fixed]
    shapes[0] = shapes[0][1:]
    col_v, row_v, side_v, half_v, field_v, spread_v, across_v, kernels_v = pl.pallas_call(
        staging,
        out_shape=[jax.ShapeDtypeStruct(z, jnp.bfloat16) for z in shapes],
        in_specs=[hbm] * len(fixed),
        out_specs=[vmem] * len(fixed),
        scratch_shapes=[pltpu.SemaphoreType.DMA((len(fixed),))],
        compiler_params=params,
        name="staging",
    )(*map(in_hbm, fixed))
    part = pl.pallas_call(
        row_analysis,
        out_shape=jax.ShapeDtypeStruct((2 * band, half + wide), jnp.float32),
        in_specs=[hbm, vmem, vmem],
        out_specs=vmem,
        scratch_shapes=[pltpu.VMEM((core, half), jnp.bfloat16), pltpu.SemaphoreType.DMA],
        compiler_params=params,
        name="row_analysis",
    )(in_hbm(tile), strip, row_v)
    mine = pl.pallas_call(
        lambda *refs: spectrum(*refs, sides=sides),
        out_shape=jax.ShapeDtypeStruct((band, grid), jnp.float32),
        in_specs=[vmem] * (3 + len(uprights)),
        out_specs=vmem,
        compiler_params=params,
        name="spectrum",
    )(part, side_v, col_v, *uprights)
    other = lax.ppermute(mine, "cond", [(0, 1), (1, 0)])
    send, level, gain = pl.pallas_call(
        lambda *refs: imaging(*refs, pad=pad),
        out_shape=(
            jax.ShapeDtypeStruct((2, share, core), jnp.bfloat16),
            jax.ShapeDtypeStruct((2, conds * grid, core), jnp.bfloat16),
            jax.ShapeDtypeStruct((2, conds, 8, core), jnp.float32),
        ),
        in_specs=[hbm] * 3 + [vmem] * 7,
        out_specs=(vmem, vmem, vmem),
        scratch_shapes=[
            pltpu.VMEM((kerns * band, 2 * grid), jnp.bfloat16),
            pltpu.VMEM((conds, grid, grid), jnp.float32),
            pltpu.SMEM(socs_weight.shape, jnp.float32),
            pltpu.SMEM(dose.shape, jnp.float32),
            pltpu.SMEM(threshold.shape, jnp.float32),
            pltpu.SemaphoreType.DMA((3,)),
        ],
        compiler_params=params,
        name="imaging",
    )(
        in_hbm(socs_weight),
        in_hbm(dose),
        in_hbm(threshold),
        mine,
        other,
        half_v,
        field_v,
        spread_v,
        across_v,
        kernels_v,
    )
    other = lax.ppermute(send, "cond", [(0, 1), (1, 0)])
    keep = pl.pallas_call(
        own_share,
        out_shape=jax.ShapeDtypeStruct((2, share, core), jnp.float32),
        in_specs=[vmem] * 3,
        out_specs=vmem,
        compiler_params=params,
        name="own_share",
    )(level, gain, spread_v)
    other = other.astype(jnp.float32)
    return (jnp.maximum(keep[0], other[0])[None], jnp.minimum(keep[1], other[1])[None])


def solution(mesh):
    return jax.shard_map(
        on_device,
        mesh=mesh,
        in_specs=(
            P(("parts", "tile"), None, None),
            P("cond", None, None, None),
            P("cond", None),
            P("cond"),
            P("cond"),
        ),
        out_specs=(P(("parts", "tile"), "cond", None), P(("parts", "tile"), "cond", None)),
        check_vma=False,
    )
```

```python
import math

import jax
import jax.numpy as jnp
import numpy as np
from jax import lax
from jax.experimental import pallas as pl
from jax.experimental.pallas import tpu as pltpu
from jax.sharding import PartitionSpec as P

MARGIN = 64
BLUR = 8

diffusion = 2.0
steepness = 8.0


def phases(pixels, freqs, period):
    angle = 2.0 * np.pi * ((pixels[:, None] * freqs[None, :]) % period) / period
    return np.cos(angle), np.sin(angle)


def make_tables(core, band):
    pad = core + 2 * MARGIN
    freqs = np.arange(band) - band // 2
    cos_in, sin_in = phases(np.arange(pad), freqs, pad)
    row_all = np.concatenate([cos_in, -sin_in], axis=1).T
    row_core = row_all[:, MARGIN : MARGIN + core]
    row_side = np.stack([row_all[:, :MARGIN], row_all[:, MARGIN + core :]])
    table = np.stack(
        [np.concatenate([cos_in, -sin_in], axis=1), np.concatenate([sin_in, cos_in], axis=1)]
    )
    none = np.zeros((2, MARGIN, 2 * band))
    half = core // 2
    middle = MARGIN + half
    columns = np.stack(
        [
            np.concatenate([table[:, MARGIN:middle], none, table[:, :MARGIN]], axis=1),
            np.concatenate([table[:, middle : middle + half], table[:, -MARGIN:], none], axis=1),
        ]
    )
    grid = 2 * band
    cos_g, sin_g = phases(np.arange(grid), freqs, grid)
    half_table = np.concatenate(
        [np.concatenate([cos_g.T, sin_g.T], axis=1), np.concatenate([-sin_g.T, cos_g.T], axis=1)],
        axis=0,
    )
    field_table = np.concatenate(
        [np.concatenate([cos_g, -sin_g], axis=1), np.concatenate([sin_g, cos_g], axis=1)], axis=0
    )
    pixel = np.arange(core + 2 * BLUR) + MARGIN - BLUR
    sample = np.arange(grid) * (pad / grid)
    degrees = np.arange(1, grid // 2)
    gap = pixel[:, None] - sample[None, :]
    interp = (
        1.0 + 2.0 * np.cos(2.0 * np.pi * gap[:, :, None] * degrees / pad).sum(axis=-1)
    ) / grid
    offset = np.arange(core + 2 * BLUR)[None, :] - np.arange(core)[:, None] - BLUR
    taps = np.where(
        np.abs(offset) <= BLUR, np.exp(-(offset**2) / (2.0 * diffusion * diffusion)), 0.0
    )
    reach = np.arange(-BLUR, BLUR + 1)
    taps = taps / np.exp(-(reach**2) / (2.0 * diffusion * diffusion)).sum()
    spread = taps @ interp
    return row_core, row_side, columns, half_table, field_table, spread


def split(value):
    high = value.astype(jnp.bfloat16)
    low = (value - high.astype(jnp.float32)).astype(jnp.bfloat16)
    return high, low


def dot(a, b):
    return jnp.dot(a, b, preferred_element_type=jnp.float32)


def placement():
    count = lax.axis_size("tile")
    columns = min(8, count // 2)
    grid_rows = count // columns
    position = (lax.axis_index("tile") + columns // 2) % count
    column = position % columns
    row = position // columns
    return dict(
        columns=columns,
        grid_rows=grid_rows,
        right=column < columns - 1,
        left=column > 0,
        above=row > 0,
        below=row < grid_rows - 1,
        top=row == 0,
        half=lax.axis_index("cond"),
    )


def dma_all(pairs, sems):
    return [pltpu.make_async_copy(src, dst, sems.at[n]) for n, (src, dst) in enumerate(pairs)]


def staging(*refs, count):
    tile_hbm, weight_hbm, dose_hbm, threshold_hbm, columns_hbm = refs[:5]
    sources = refs[5 : count + 4]
    columns_ref, *targets = refs[count + 4 : 2 * count + 4]
    tile_ref, part_ref, share_ref, gain_ref, weight_ref, dose_ref, threshold_ref, sems = refs[
        2 * count + 4 :
    ]
    core, half = tile_ref.shape
    own = lax.axis_index("cond")
    first = pl.multiple_of(own * half, half)
    pairs = [
        (weight_hbm, weight_ref),
        (dose_hbm, dose_ref),
        (threshold_hbm, threshold_ref),
        (tile_hbm.at[:, pl.ds(first, half)], tile_ref),
        *zip(sources, targets),
        (columns_hbm.at[own], columns_ref),
    ]
    copies = dma_all(pairs, sems)
    for copy in copies:
        copy.start()
    for copy in copies[:5]:
        copy.wait()
    row_core_ref = targets[0]
    part_ref[...] = dot(row_core_ref[...], tile_ref[...])
    conds, kerns = weight_hbm.shape
    scale = float(row_core_ref.shape[0] // 2) ** 2
    for c in range(conds):
        mass = weight_ref[c, 0]
        for k in range(kerns):
            mass = mass + weight_ref[c, k] if k else mass
            share_ref[c * kerns + k, :] = jnp.full((share_ref.shape[1],), weight_ref[c, k])
        gain_ref[0, c] = steepness * dose_ref[c] / jnp.full((8, core), mass * scale)
        gain_ref[1, c] = jnp.full((8, core), steepness * threshold_ref[c])
    for copy in copies[5:]:
        copy.wait()


def pack(tile_ref, strip_ref, *out_refs, sides):
    core, half = tile_ref.shape
    for side, out_ref in zip(sides, out_refs):
        if side is None:
            lower = placement()["top"].astype(jnp.int32)
            first = pl.multiple_of(lower * (core - MARGIN), MARGIN)
        else:
            first = 0 if side else core - MARGIN
        out_ref[:, :half] = tile_ref[pl.ds(first, MARGIN)]
        out_ref[:, half:] = strip_ref[pl.ds(first, MARGIN)]


def edge_analysis(row_core_ref, strip_ref, part_ref):
    part_ref[...] = dot(row_core_ref[...], strip_ref[...])


def spectrum(core_ref, edge_ref, row_side_ref, columns_ref, *rest, sides):
    *upright_refs, spec_ref = rest
    place = placement()
    band = spec_ref.shape[0]
    half = core_ref.shape[1]
    part = jnp.concatenate([core_ref[...], edge_ref[...]], axis=1)
    for n, side in enumerate(sides):
        if side is None:
            table = row_side_ref[place["top"].astype(jnp.int32)]
            part = part + dot(table, upright_refs[n][...])
        else:
            there = place["below"] if side else place["above"]
            more = dot(row_side_ref[side], upright_refs[n][...])
            part = part + jnp.where(there, more, jnp.zeros_like(more))
    edge = part[:, half:]
    beside = jnp.where(place["half"] == 0, place["left"], place["right"])
    edge = jnp.where(beside, edge, jnp.zeros_like(edge))
    part = jnp.concatenate([part[:, :half], edge], axis=1).astype(jnp.bfloat16)
    spec_ref[...] = dot(part[:band], columns_ref[0]) + dot(part[band:], columns_ref[1])


def imaging(
    mine_ref,
    other_ref,
    half_ref,
    field_ref,
    spread_ref,
    across_ref,
    kern_ref,
    share_ref,
    gain_ref,
    send_ref,
    level_ref,
    halves_ref,
    coarse_ref,
    *,
    pad,
):
    conds, kerns, band, _ = kern_ref.shape
    grid = 2 * band
    core = spread_ref.shape[1]
    spec = (mine_ref[...] + other_ref[...]) * (1.0 / pad)
    swapped = pltpu.roll(spec, band, 1)
    first = lax.broadcasted_iota(jnp.int32, spec.shape, 1) < band
    spec_same = jnp.where(first, spec, swapped)
    spec_cross = jnp.where(first, -swapped, spec)

    def condition(c, carry):
        prods = []
        for k in range(kerns):
            kern = kern_ref[c, k].astype(jnp.float32)
            prod = kern * spec_same + pltpu.roll(kern, band, 1) * spec_cross
            prods.append(prod.astype(jnp.bfloat16))
        halves_ref[...] = dot(jnp.concatenate(prods, axis=0), half_ref[...]).astype(jnp.bfloat16)
        total = jnp.zeros((grid, grid), jnp.float32)
        for k in range(0, kerns, 2):
            a = halves_ref[k * band : (k + 1) * band]
            b = halves_ref[(k + 1) * band : (k + 2) * band]
            both = jnp.concatenate(
                [
                    jnp.concatenate([a[:, :grid], b[:, :grid]], axis=1),
                    jnp.concatenate([a[:, grid:], b[:, grid:]], axis=1),
                ],
                axis=0,
            )
            field = dot(field_ref[...], both)
            power = field[:grid] * field[:grid] + field[grid:] * field[grid:]
            shares = share_ref[pl.ds(c * kerns + k, 1)], share_ref[pl.ds(c * kerns + k + 1, 1)]
            total = total + shares[0] * power[:, :grid] + shares[1] * power[:, grid:]
        coarse_ref[c] = total
        return carry

    lax.fori_loop(0, conds, condition, 0)
    high, low = split(coarse_ref[...].reshape(conds * grid, grid))
    across = dot(high, across_ref[0]) + dot(low, across_ref[0]) + dot(high, across_ref[1])
    level_ref[0], level_ref[1] = split(across)
    most, least = band_of(1 - lax.axis_index("cond"), level_ref, gain_ref, spread_ref)
    send_ref[0] = most.astype(jnp.bfloat16)
    send_ref[1] = least.astype(jnp.bfloat16)


def band_of(part_of, level_ref, gain_ref, spread_ref):
    conds = gain_ref.shape[1]
    core = spread_ref.shape[1]
    grid = level_ref.shape[1] // conds
    share = core // 2
    rows = pl.ds(pl.multiple_of(part_of * share, share), share)
    for c in range(conds):
        h = level_ref[0, c * grid : (c + 1) * grid]
        l = level_ref[1, c * grid : (c + 1) * grid]
        blurred = dot(spread_ref[0, rows], h)
        blurred = blurred + dot(spread_ref[0, rows], l) + dot(spread_ref[1, rows], h)
        level = gain_ref[0, c, :1] * blurred - gain_ref[1, c, :1]
        most = level if c == 0 else jnp.maximum(most, level)
        least = level if c == 0 else jnp.minimum(least, level)
    return jax.nn.sigmoid(most), jax.nn.sigmoid(least)


def own_share(level_ref, gain_ref, spread_ref, keep_ref):
    keep_ref[0], keep_ref[1] = band_of(lax.axis_index("cond"), level_ref, gain_ref, spread_ref)


def two_parts(table):
    high = np.asarray(table, np.float32).astype(jnp.bfloat16)
    low = (table - high.astype(np.float64)).astype(jnp.bfloat16)
    return np.stack([high, low])


def in_hbm(value):
    return pltpu.with_memory_space_constraint(value, pltpu.HBM)


def shifted(block, axis, distance):
    count = lax.axis_size(axis)
    return lax.ppermute(block, axis, [((i - distance) % count, i) for i in range(count)])


def on_device(mask, kernels, socs_weight, dose, threshold):
    tile = mask[0]
    core = tile.shape[0]
    conds, kerns, band, _ = kernels.shape
    pad = core + 2 * MARGIN
    grid = 2 * band
    place = placement()
    count = lax.axis_size("tile")
    columns, grid_rows = place["columns"], place["grid_rows"]

    half, wide = core // 2, 2 * MARGIN
    left_core = lax.axis_index("cond") == 0
    others = [((t - 1) % count, t) for t in range(count)]
    route = [(2 * a, 2 * b) for a, b in others] + [(2 * b + 1, 2 * a + 1) for a, b in others]
    strip = lax.ppermute(
        jnp.where(left_core, tile[:, -wide:], tile[:, :wide]), ("tile", "cond"), route
    )
    sides = (None,) if grid_rows == 2 else (0, 1)
    row_core, row_side, col_table, half_t, field_t, spread = make_tables(core, band)
    bf = lambda t: jnp.asarray(np.asarray(t).astype(jnp.bfloat16))
    fixed = [
        bf(col_table),
        bf(row_core),
        bf(row_side),
        bf(half_t),
        bf(field_t),
        jnp.asarray(two_parts(spread)),
        jnp.asarray(two_parts(spread.T)),
        kernels,
    ]
    vmem = pl.BlockSpec(memory_space=pltpu.VMEM)
    hbm = pl.BlockSpec(memory_space=pltpu.HBM)
    share = core // lax.axis_size("cond")
    params = pltpu.CompilerParams(vmem_limit_bytes=16 * 2**20)
    outs = [jax.ShapeDtypeStruct(t.shape, t.dtype) for t in fixed]
    outs[0] = jax.ShapeDtypeStruct(fixed[0].shape[1:], fixed[0].dtype)
    outs += [
        jax.ShapeDtypeStruct((core, half), tile.dtype),
        jax.ShapeDtypeStruct((2 * band, half), jnp.float32),
        jax.ShapeDtypeStruct((conds * kerns, grid), jnp.float32),
        jax.ShapeDtypeStruct((2, conds, 8, core), jnp.float32),
    ]
    scalars = (socs_weight, dose, threshold)
    (col_v, row_v, side_v, half_v, field_v, spread_v, across_v, kernels_v, tile_v, part, *gains) = (
        pl.pallas_call(
            lambda *refs: staging(*refs, count=len(fixed)),
            out_shape=outs,
            in_specs=[hbm] * (4 + len(fixed)),
            out_specs=[vmem] * len(outs),
            scratch_shapes=[pltpu.SMEM(t.shape, t.dtype) for t in scalars]
            + [pltpu.SemaphoreType.DMA((4 + len(fixed),))],
            compiler_params=params,
            name="staging",
        )(*map(in_hbm, (tile, *scalars, *fixed)))
    )
    block = jax.ShapeDtypeStruct((MARGIN, half + wide), tile.dtype)
    blocks = pl.pallas_call(
        lambda *refs: pack(*refs, sides=sides),
        out_shape=[block] * len(sides),
        in_specs=[vmem, vmem],
        out_specs=[vmem] * len(sides),
        compiler_params=params,
        name="pack",
    )(tile_v, strip)
    uprights = [
        shifted(t, "tile", -columns if side else columns) for t, side in zip(blocks, sides)
    ]
    edge = pl.pallas_call(
        edge_analysis,
        out_shape=jax.ShapeDtypeStruct((2 * band, wide), jnp.float32),
        in_specs=[vmem, vmem],
        out_specs=vmem,
        compiler_params=params,
        name="edge_analysis",
    )(row_v, strip)
    mine = pl.pallas_call(
        lambda *refs: spectrum(*refs, sides=sides),
        out_shape=jax.ShapeDtypeStruct((band, grid), jnp.float32),
        in_specs=[vmem] * (4 + len(uprights)),
        out_specs=vmem,
        compiler_params=params,
        name="spectrum",
    )(part, edge, side_v, col_v, *uprights)
    other = lax.ppermute(mine, "cond", [(0, 1), (1, 0)])
    send, level = pl.pallas_call(
        lambda *refs: imaging(*refs, pad=pad),
        out_shape=(
            jax.ShapeDtypeStruct((2, share, core), jnp.bfloat16),
            jax.ShapeDtypeStruct((2, conds * grid, core), jnp.bfloat16),
        ),
        in_specs=[vmem] * 9,
        out_specs=(vmem, vmem),
        scratch_shapes=[
            pltpu.VMEM((kerns * band, 2 * grid), jnp.bfloat16),
            pltpu.VMEM((conds, grid, grid), jnp.float32),
        ],
        compiler_params=params,
        name="imaging",
    )(mine, other, half_v, field_v, spread_v, across_v, kernels_v, *gains)
    other = lax.ppermute(send, "cond", [(0, 1), (1, 0)])
    keep = pl.pallas_call(
        own_share,
        out_shape=jax.ShapeDtypeStruct((2, share, core), jnp.float32),
        in_specs=[vmem] * 3,
        out_specs=vmem,
        compiler_params=params,
        name="own_share",
    )(level, gains[1], spread_v)
    other = other.astype(jnp.float32)
    return (jnp.maximum(keep[0], other[0])[None], jnp.minimum(keep[1], other[1])[None])


def solution(mesh):
    return jax.shard_map(
        on_device,
        mesh=mesh,
        in_specs=(
            P(("parts", "tile"), None, None),
            P("cond", None, None, None),
            P("cond", None),
            P("cond"),
            P("cond"),
        ),
        out_specs=(P(("parts", "tile"), "cond", None), P(("parts", "tile"), "cond", None)),
        check_vma=False,
    )
```

```python
import math

import jax
import jax.numpy as jnp
import numpy as np
from jax import lax
from jax.experimental import pallas as pl
from jax.experimental.pallas import tpu as pltpu
from jax.sharding import PartitionSpec as P

MARGIN = 64
BLUR = 8

diffusion = 2.0
steepness = 8.0


def phases(pixels, freqs, period):
    angle = 2.0 * np.pi * ((pixels[:, None] * freqs[None, :]) % period) / period
    return np.cos(angle), np.sin(angle)


def make_tables(core, band):
    pad = core + 2 * MARGIN
    freqs = np.arange(band) - band // 2
    cos_in, sin_in = phases(np.arange(pad), freqs, pad)
    row_all = np.concatenate([cos_in, -sin_in], axis=1).T
    row_core = row_all[:, MARGIN : MARGIN + core]
    row_side = np.stack([row_all[:, :MARGIN].T, row_all[:, MARGIN + core :].T])
    table = np.stack(
        [np.concatenate([cos_in, -sin_in], axis=1), np.concatenate([sin_in, cos_in], axis=1)]
    )
    none = np.zeros((2, MARGIN, 2 * band))
    half = core // 2
    middle = MARGIN + half
    columns = np.stack(
        [
            np.concatenate([table[:, MARGIN:middle], none, table[:, :MARGIN]], axis=1),
            np.concatenate([table[:, middle : middle + half], table[:, -MARGIN:], none], axis=1),
        ]
    )
    grid = 2 * band
    cos_g, sin_g = phases(np.arange(grid), freqs, grid)
    half_table = np.concatenate(
        [np.concatenate([cos_g.T, sin_g.T], axis=1), np.concatenate([-sin_g.T, cos_g.T], axis=1)],
        axis=0,
    )
    field_table = np.concatenate(
        [np.concatenate([cos_g, -sin_g], axis=1), np.concatenate([sin_g, cos_g], axis=1)], axis=0
    )
    pixel = np.arange(core + 2 * BLUR) + MARGIN - BLUR
    sample = np.arange(grid) * (pad / grid)
    degrees = np.arange(1, grid // 2)
    gap = pixel[:, None] - sample[None, :]
    interp = (
        1.0 + 2.0 * np.cos(2.0 * np.pi * gap[:, :, None] * degrees / pad).sum(axis=-1)
    ) / grid
    offset = np.arange(core + 2 * BLUR)[None, :] - np.arange(core)[:, None] - BLUR
    taps = np.where(
        np.abs(offset) <= BLUR, np.exp(-(offset**2) / (2.0 * diffusion * diffusion)), 0.0
    )
    reach = np.arange(-BLUR, BLUR + 1)
    taps = taps / np.exp(-(reach**2) / (2.0 * diffusion * diffusion)).sum()
    spread = taps @ interp
    return row_core, row_side, columns, half_table, field_table, spread


def split(value):
    high = value.astype(jnp.bfloat16)
    low = (value - high.astype(jnp.float32)).astype(jnp.bfloat16)
    return high, low


def dot(a, b):
    return jnp.dot(a, b, preferred_element_type=jnp.float32)


def placement():
    count = lax.axis_size("tile")
    columns = min(8, count // 2)
    grid_rows = count // columns
    position = (lax.axis_index("tile") + columns // 2) % count
    column = position % columns
    row = position // columns
    return dict(
        columns=columns,
        grid_rows=grid_rows,
        right=column < columns - 1,
        left=column > 0,
        above=row > 0,
        below=row < grid_rows - 1,
        top=row == 0,
        half=lax.axis_index("cond"),
    )


def dot_first(a, b):
    return lax.dot_general(a, b, (((0,), (0,)), ((), ())), preferred_element_type=jnp.float32)


def native_lanes(shape):
    upper = (lax.broadcasted_iota(jnp.int32, shape, 1) >= MARGIN).astype(jnp.int32)
    return upper != lax.axis_index("cond")


def folded(block):
    rows = block.shape[0] // 2
    block = block.astype(jnp.float32)
    back = pltpu.roll(block[rows:], MARGIN, 1)
    return jnp.where(native_lanes(back.shape), block[:rows], back).astype(jnp.bfloat16)


def dma_all(pairs, sems):
    return [pltpu.make_async_copy(src, dst, sems.at[n]) for n, (src, dst) in enumerate(pairs)]


def staging(*refs, count):
    tile_hbm, weight_hbm, dose_hbm, threshold_hbm, columns_hbm = refs[:5]
    sources = refs[5 : count + 4]
    columns_ref, *targets = refs[count + 4 : 2 * count + 4]
    tile_ref, part_ref, share_ref, gain_ref, weight_ref, dose_ref, threshold_ref, sems = refs[
        2 * count + 4 :
    ]
    core, half = tile_ref.shape
    own = lax.axis_index("cond")
    first = pl.multiple_of(own * half, half)
    pairs = [
        (weight_hbm, weight_ref),
        (dose_hbm, dose_ref),
        (threshold_hbm, threshold_ref),
        (tile_hbm.at[:, pl.ds(first, half)], tile_ref),
        *zip(sources, targets),
        (columns_hbm.at[own], columns_ref),
    ]
    copies = dma_all(pairs, sems)
    for copy in copies:
        copy.start()
    for copy in copies[:5]:
        copy.wait()
    row_core_ref = targets[0]
    part_ref[...] = dot(row_core_ref[...], tile_ref[...])
    conds, kerns = weight_hbm.shape
    scale = float(row_core_ref.shape[0] // 2) ** 2
    for c in range(conds):
        mass = weight_ref[c, 0]
        for k in range(kerns):
            mass = mass + weight_ref[c, k] if k else mass
            share_ref[c * kerns + k, :] = jnp.full((share_ref.shape[1],), weight_ref[c, k])
        gain_ref[0, c] = steepness * dose_ref[c] / jnp.full((8, core), mass * scale)
        gain_ref[1, c] = jnp.full((8, core), steepness * threshold_ref[c])
    for copy in copies[5:]:
        copy.wait()


def cut(tile_hbm, strip_ref, *refs, sides):
    upright_refs, corner_refs = refs[: len(sides)], refs[len(sides) : 2 * len(sides)]
    block_ref, sems = refs[2 * len(sides) :]
    core, wide = block_ref.shape
    half = upright_refs[0].shape[1]
    own = lax.axis_index("cond")
    beside = pl.multiple_of((1 - own) * (core - wide), wide)
    first = pl.multiple_of(own * half, half)
    rows = []
    for side in sides:
        if side is None:
            lower = placement()["top"].astype(jnp.int32)
            rows.append(pl.ds(pl.multiple_of(lower * (core - MARGIN), MARGIN), MARGIN))
        else:
            rows.append(pl.ds(0 if side else core - MARGIN, MARGIN))
    pairs = [(tile_hbm.at[:, pl.ds(beside, wide)], block_ref)]
    for r, upright_ref in zip(rows, upright_refs):
        pairs.append((tile_hbm.at[r, pl.ds(first, half)], upright_ref))
    copies = dma_all(pairs, sems)
    for copy in copies:
        copy.start()
    copies[0].wait()
    strip_ref[...] = folded(block_ref[...])
    for r, corner_ref in zip(rows, corner_refs):
        corner_ref[...] = folded(block_ref[r])
    for copy in copies[1:]:
        copy.wait()


def spectrum(core_ref, row_core_ref, row_side_ref, columns_ref, strip_ref, *rest, sides):
    upright_refs, corner_refs = rest[: len(sides)], rest[len(sides) : 2 * len(sides)]
    spec_ref = rest[-1]
    place = placement()
    band = spec_ref.shape[0]
    fold = strip_ref.shape[0]
    fold_side = corner_refs[0].shape[0]
    core = core_ref[...]
    ahead = dot(row_core_ref[:, :fold], strip_ref[...])
    behind = dot(row_core_ref[:, fold:], strip_ref[...])
    for n, side in enumerate(sides):
        table = row_side_ref.at[place["top"].astype(jnp.int32) if side is None else side]
        more = (
            dot_first(table[...], upright_refs[n][...]),
            dot_first(table[:fold_side], corner_refs[n][...]),
            dot_first(table[fold_side:], corner_refs[n][...]),
        )
        if side is not None:
            there = place["below"] if side else place["above"]
            more = [jnp.where(there, m, jnp.zeros_like(m)) for m in more]
        core, ahead, behind = core + more[0], ahead + more[1], behind + more[2]
    edge = ahead + pltpu.roll(behind, MARGIN, 1)
    beside = jnp.where(place["half"] == 0, place["left"], place["right"])
    edge = jnp.where(beside, edge, jnp.zeros_like(edge))
    part = jnp.concatenate([core, edge], axis=1).astype(jnp.bfloat16)
    spec_ref[...] = dot(part[:band], columns_ref[0]) + dot(part[band:], columns_ref[1])


def imaging(
    mine_ref,
    other_ref,
    half_ref,
    field_ref,
    spread_ref,
    across_ref,
    kern_ref,
    share_ref,
    gain_ref,
    send_ref,
    level_ref,
    halves_ref,
    coarse_ref,
    *,
    pad,
):
    conds, kerns, band, _ = kern_ref.shape
    grid = 2 * band
    core = spread_ref.shape[1]
    spec = (mine_ref[...] + other_ref[...]) * (1.0 / pad)
    swapped = pltpu.roll(spec, band, 1)
    first = lax.broadcasted_iota(jnp.int32, spec.shape, 1) < band
    spec_same = jnp.where(first, spec, swapped)
    spec_cross = jnp.where(first, -swapped, spec)

    def condition(c, carry):
        prods = []
        for k in range(kerns):
            kern = kern_ref[c, k].astype(jnp.float32)
            prod = kern * spec_same + pltpu.roll(kern, band, 1) * spec_cross
            prods.append(prod.astype(jnp.bfloat16))
        halves_ref[...] = dot(jnp.concatenate(prods, axis=0), half_ref[...]).astype(jnp.bfloat16)
        total = jnp.zeros((grid, grid), jnp.float32)
        for k in range(0, kerns, 2):
            a = halves_ref[k * band : (k + 1) * band]
            b = halves_ref[(k + 1) * band : (k + 2) * band]
            both = jnp.concatenate(
                [
                    jnp.concatenate([a[:, :grid], b[:, :grid]], axis=1),
                    jnp.concatenate([a[:, grid:], b[:, grid:]], axis=1),
                ],
                axis=0,
            )
            field = dot(field_ref[...], both)
            power = field[:grid] * field[:grid] + field[grid:] * field[grid:]
            shares = share_ref[pl.ds(c * kerns + k, 1)], share_ref[pl.ds(c * kerns + k + 1, 1)]
            total = total + shares[0] * power[:, :grid] + shares[1] * power[:, grid:]
        coarse_ref[c] = total
        return carry

    lax.fori_loop(0, conds, condition, 0)
    high, low = split(coarse_ref[...].reshape(conds * grid, grid))
    across = dot(high, across_ref[0]) + dot(low, across_ref[0]) + dot(high, across_ref[1])
    level_ref[0], level_ref[1] = split(across)
    most, least = band_of(1 - lax.axis_index("cond"), level_ref, gain_ref, spread_ref)
    send_ref[0] = most.astype(jnp.bfloat16)
    send_ref[1] = least.astype(jnp.bfloat16)


def band_of(part_of, level_ref, gain_ref, spread_ref):
    conds = gain_ref.shape[1]
    core = spread_ref.shape[1]
    grid = level_ref.shape[1] // conds
    share = core // 2
    rows = pl.ds(pl.multiple_of(part_of * share, share), share)
    for c in range(conds):
        h = level_ref[0, c * grid : (c + 1) * grid]
        l = level_ref[1, c * grid : (c + 1) * grid]
        blurred = dot(spread_ref[0, rows], h)
        blurred = blurred + dot(spread_ref[0, rows], l) + dot(spread_ref[1, rows], h)
        level = gain_ref[0, c, :1] * blurred - gain_ref[1, c, :1]
        most = level if c == 0 else jnp.maximum(most, level)
        least = level if c == 0 else jnp.minimum(least, level)
    return jax.nn.sigmoid(most), jax.nn.sigmoid(least)


def own_share(level_ref, gain_ref, spread_ref, keep_ref):
    keep_ref[0], keep_ref[1] = band_of(lax.axis_index("cond"), level_ref, gain_ref, spread_ref)


def two_parts(table):
    high = np.asarray(table, np.float32).astype(jnp.bfloat16)
    low = (table - high.astype(np.float64)).astype(jnp.bfloat16)
    return np.stack([high, low])


def in_hbm(value):
    return pltpu.with_memory_space_constraint(value, pltpu.HBM)


def shifted(block, axis, distance):
    count = lax.axis_size(axis)
    return lax.ppermute(block, axis, [((i - distance) % count, i) for i in range(count)])


def on_device(mask, kernels, socs_weight, dose, threshold):
    tile = mask[0]
    core = tile.shape[0]
    conds, kerns, band, _ = kernels.shape
    pad = core + 2 * MARGIN
    grid = 2 * band
    place = placement()
    count = lax.axis_size("tile")
    columns, grid_rows = place["columns"], place["grid_rows"]

    half, wide = core // 2, 2 * MARGIN
    sides = (None,) if grid_rows == 2 else (0, 1)
    vmem = pl.BlockSpec(memory_space=pltpu.VMEM)
    hbm = pl.BlockSpec(memory_space=pltpu.HBM)
    params = pltpu.CompilerParams(vmem_limit_bytes=16 * 2**20)
    strip, *blocks = pl.pallas_call(
        lambda *refs: cut(*refs, sides=sides),
        out_shape=[jax.ShapeDtypeStruct((core // 2, wide), tile.dtype)]
        + [jax.ShapeDtypeStruct((MARGIN, half), tile.dtype)] * len(sides)
        + [jax.ShapeDtypeStruct((MARGIN // 2, wide), tile.dtype)] * len(sides),
        in_specs=[hbm],
        out_specs=[vmem] * (1 + 2 * len(sides)),
        scratch_shapes=[
            pltpu.VMEM((core, wide), tile.dtype),
            pltpu.SemaphoreType.DMA((1 + len(sides),)),
        ],
        compiler_params=params,
        name="cut",
    )(in_hbm(tile))

    def passed(block, shift):
        pairs = []
        for t in range(count):
            pairs.append((2 * ((t - shift - 1) % count), 2 * t))
            pairs.append((2 * ((t - shift + 1) % count) + 1, 2 * t + 1))
        return lax.ppermute(block, ("tile", "cond"), pairs)

    shifts = [-columns if side else columns for side in sides]
    strip = passed(strip, 0)
    corners = [passed(t, d) for t, d in zip(blocks[len(sides) :], shifts)]
    uprights = [shifted(t, "tile", d) for t, d in zip(blocks, shifts)]
    row_core, row_side, col_table, half_t, field_t, spread = make_tables(core, band)
    bf = lambda t: jnp.asarray(np.asarray(t).astype(jnp.bfloat16))
    fixed = [
        bf(col_table),
        bf(row_core),
        bf(row_side),
        bf(half_t),
        bf(field_t),
        jnp.asarray(two_parts(spread)),
        jnp.asarray(two_parts(spread.T)),
        kernels,
    ]
    share = core // lax.axis_size("cond")
    outs = [jax.ShapeDtypeStruct(t.shape, t.dtype) for t in fixed]
    outs[0] = jax.ShapeDtypeStruct(fixed[0].shape[1:], fixed[0].dtype)
    outs += [
        jax.ShapeDtypeStruct((core, half), tile.dtype),
        jax.ShapeDtypeStruct((2 * band, half), jnp.float32),
        jax.ShapeDtypeStruct((conds * kerns, grid), jnp.float32),
        jax.ShapeDtypeStruct((2, conds, 8, core), jnp.float32),
    ]
    scalars = (socs_weight, dose, threshold)
    (col_v, row_v, side_v, half_v, field_v, spread_v, across_v, kernels_v, tile_v, part, *gains) = (
        pl.pallas_call(
            lambda *refs: staging(*refs, count=len(fixed)),
            out_shape=outs,
            in_specs=[hbm] * (4 + len(fixed)),
            out_specs=[vmem] * len(outs),
            scratch_shapes=[pltpu.SMEM(t.shape, t.dtype) for t in scalars]
            + [pltpu.SemaphoreType.DMA((4 + len(fixed),))],
            compiler_params=params,
            name="staging",
        )(*map(in_hbm, (tile, *scalars, *fixed)))
    )
    mine = pl.pallas_call(
        lambda *refs: spectrum(*refs, sides=sides),
        out_shape=jax.ShapeDtypeStruct((band, grid), jnp.float32),
        in_specs=[vmem] * (5 + 2 * len(sides)),
        out_specs=vmem,
        compiler_params=params,
        name="spectrum",
    )(part, row_v, side_v, col_v, strip, *uprights, *corners)
    other = lax.ppermute(mine, "cond", [(0, 1), (1, 0)])
    send, level = pl.pallas_call(
        lambda *refs: imaging(*refs, pad=pad),
        out_shape=(
            jax.ShapeDtypeStruct((2, share, core), jnp.bfloat16),
            jax.ShapeDtypeStruct((2, conds * grid, core), jnp.bfloat16),
        ),
        in_specs=[vmem] * 9,
        out_specs=(vmem, vmem),
        scratch_shapes=[
            pltpu.VMEM((kerns * band, 2 * grid), jnp.bfloat16),
            pltpu.VMEM((conds, grid, grid), jnp.float32),
        ],
        compiler_params=params,
        name="imaging",
    )(mine, other, half_v, field_v, spread_v, across_v, kernels_v, *gains)
    other = lax.ppermute(send, "cond", [(0, 1), (1, 0)])
    keep = pl.pallas_call(
        own_share,
        out_shape=jax.ShapeDtypeStruct((2, share, core), jnp.float32),
        in_specs=[vmem] * 3,
        out_specs=vmem,
        compiler_params=params,
        name="own_share",
    )(level, gains[1], spread_v)
    other = other.astype(jnp.float32)
    return (jnp.maximum(keep[0], other[0])[None], jnp.minimum(keep[1], other[1])[None])


def solution(mesh):
    return jax.shard_map(
        on_device,
        mesh=mesh,
        in_specs=(
            P(("parts", "tile"), None, None),
            P("cond", None, None, None),
            P("cond", None),
            P("cond"),
            P("cond"),
        ),
        out_specs=(P(("parts", "tile"), "cond", None), P(("parts", "tile"), "cond", None)),
        check_vma=False,
    )
```

```python
import math

import jax
import jax.numpy as jnp
import numpy as np
from jax import lax
from jax.experimental import pallas as pl
from jax.experimental.pallas import tpu as pltpu
from jax.sharding import PartitionSpec as P

MARGIN = 64
BLUR = 8

diffusion = 2.0
steepness = 8.0


def phases(pixels, freqs, period):
    angle = 2.0 * np.pi * ((pixels[:, None] * freqs[None, :]) % period) / period
    return np.cos(angle), np.sin(angle)


def make_tables(core, band):
    pad = core + 2 * MARGIN
    freqs = np.arange(band) - band // 2
    cos_in, sin_in = phases(np.arange(pad), freqs, pad)
    row_all = np.concatenate([cos_in, -sin_in], axis=1).T
    row_core = row_all[:, MARGIN : MARGIN + core]
    row_side = np.stack([row_all[:, :MARGIN].T, row_all[:, MARGIN + core :].T])
    table = np.stack(
        [np.concatenate([cos_in, -sin_in], axis=1), np.concatenate([sin_in, cos_in], axis=1)]
    )
    none = np.zeros((2, MARGIN, 2 * band))
    half = core // 2
    middle = MARGIN + half
    columns = np.stack(
        [
            np.concatenate([table[:, MARGIN:middle], none, table[:, :MARGIN]], axis=1),
            np.concatenate([table[:, middle : middle + half], table[:, -MARGIN:], none], axis=1),
        ]
    )
    grid = 2 * band
    cos_g, sin_g = phases(np.arange(grid), freqs, grid)
    half_table = np.concatenate(
        [np.concatenate([cos_g.T, sin_g.T], axis=1), np.concatenate([-sin_g.T, cos_g.T], axis=1)],
        axis=0,
    )
    field_table = np.concatenate(
        [np.concatenate([cos_g, -sin_g], axis=1), np.concatenate([sin_g, cos_g], axis=1)], axis=0
    )
    pixel = np.arange(core + 2 * BLUR) + MARGIN - BLUR
    sample = np.arange(grid) * (pad / grid)
    degrees = np.arange(1, grid // 2)
    gap = pixel[:, None] - sample[None, :]
    interp = (
        1.0 + 2.0 * np.cos(2.0 * np.pi * gap[:, :, None] * degrees / pad).sum(axis=-1)
    ) / grid
    offset = np.arange(core + 2 * BLUR)[None, :] - np.arange(core)[:, None] - BLUR
    taps = np.where(
        np.abs(offset) <= BLUR, np.exp(-(offset**2) / (2.0 * diffusion * diffusion)), 0.0
    )
    reach = np.arange(-BLUR, BLUR + 1)
    taps = taps / np.exp(-(reach**2) / (2.0 * diffusion * diffusion)).sum()
    spread = taps @ interp
    return row_core, row_side, columns, half_table, field_table, spread


def split(value):
    high = value.astype(jnp.bfloat16)
    low = (value - high.astype(jnp.float32)).astype(jnp.bfloat16)
    return high, low


def dot(a, b):
    return jnp.dot(a, b, preferred_element_type=jnp.float32)


def placement():
    count = lax.axis_size("tile")
    columns = min(8, count // 2)
    grid_rows = count // columns
    position = (lax.axis_index("tile") + columns // 2) % count
    column = position % columns
    row = position // columns
    return dict(
        columns=columns,
        grid_rows=grid_rows,
        right=column < columns - 1,
        left=column > 0,
        above=row > 0,
        below=row < grid_rows - 1,
        top=row == 0,
        half=lax.axis_index("cond"),
    )


def dot_first(a, b):
    return lax.dot_general(a, b, (((0,), (0,)), ((), ())), preferred_element_type=jnp.float32)


def native_lanes(shape):
    upper = (lax.broadcasted_iota(jnp.int32, shape, 1) >= MARGIN).astype(jnp.int32)
    return upper != lax.axis_index("cond")


def folded(block):
    rows = block.shape[0] // 2
    block = block.astype(jnp.float32)
    back = pltpu.roll(block[rows:], MARGIN, 1)
    return jnp.where(native_lanes(back.shape), block[:rows], back).astype(jnp.bfloat16)


def dma_all(pairs, sems):
    return [pltpu.make_async_copy(src, dst, sems.at[n]) for n, (src, dst) in enumerate(pairs)]


def staging(*refs, count):
    tile_hbm, weight_hbm, dose_hbm, threshold_hbm, columns_hbm = refs[:5]
    sources = refs[5 : count + 4]
    columns_ref, *targets = refs[count + 4 : 2 * count + 4]
    tile_ref, part_ref, share_ref, gain_ref, weight_ref, dose_ref, threshold_ref, sems = refs[
        2 * count + 4 :
    ]
    core, half = tile_ref.shape
    own = lax.axis_index("cond")
    first = pl.multiple_of(own * half, half)
    pairs = [
        (weight_hbm, weight_ref),
        (dose_hbm, dose_ref),
        (threshold_hbm, threshold_ref),
        (tile_hbm.at[:, pl.ds(first, half)], tile_ref),
        *zip(sources, targets),
        (columns_hbm.at[own], columns_ref),
    ]
    copies = dma_all(pairs, sems)
    for copy in copies:
        copy.start()
    for copy in copies[:5]:
        copy.wait()
    row_core_ref = targets[0]
    part_ref[...] = dot(row_core_ref[...], tile_ref[...])
    conds, kerns = weight_hbm.shape
    scale = float(row_core_ref.shape[0] // 2) ** 2
    for c in range(conds):
        mass = weight_ref[c, 0]
        for k in range(kerns):
            mass = mass + weight_ref[c, k] if k else mass
            share_ref[c * kerns + k, :] = jnp.full((share_ref.shape[1],), weight_ref[c, k])
        gain_ref[0, c] = steepness * dose_ref[c] / jnp.full((8, core), mass * scale)
        gain_ref[1, c] = jnp.full((8, core), steepness * threshold_ref[c])
    for copy in copies[5:]:
        copy.wait()


def cut(tile_hbm, strip_ref, *refs, sides):
    upright_refs, corner_refs = refs[: len(sides)], refs[len(sides) : 2 * len(sides)]
    block_ref, sems = refs[2 * len(sides) :]
    core, wide = block_ref.shape
    half = upright_refs[0].shape[1]
    own = lax.axis_index("cond")
    beside = pl.multiple_of((1 - own) * (core - wide), wide)
    first = pl.multiple_of(own * half, half)
    rows = []
    for side in sides:
        if side is None:
            lower = placement()["top"].astype(jnp.int32)
            rows.append(pl.ds(pl.multiple_of(lower * (core - MARGIN), MARGIN), MARGIN))
        else:
            rows.append(pl.ds(0 if side else core - MARGIN, MARGIN))
    pairs = [(tile_hbm.at[:, pl.ds(beside, wide)], block_ref)]
    for r, upright_ref in zip(rows, upright_refs):
        pairs.append((tile_hbm.at[r, pl.ds(first, half)], upright_ref))
    copies = dma_all(pairs, sems)
    for copy in copies:
        copy.start()
    copies[0].wait()
    strip_ref[...] = folded(block_ref[...])
    for r, corner_ref in zip(rows, corner_refs):
        corner_ref[...] = folded(block_ref[r])
    for copy in copies[1:]:
        copy.wait()


def spectrum(core_ref, row_core_ref, row_side_ref, columns_ref, strip_ref, *rest, sides):
    upright_refs, corner_refs = rest[: len(sides)], rest[len(sides) : 2 * len(sides)]
    spec_ref = rest[-1]
    place = placement()
    band = spec_ref.shape[0]
    fold = strip_ref.shape[0]
    fold_side = corner_refs[0].shape[0]
    core = core_ref[...]
    ahead = dot(row_core_ref[:, :fold], strip_ref[...])
    behind = dot(row_core_ref[:, fold:], strip_ref[...])
    for n, side in enumerate(sides):
        table = row_side_ref.at[place["top"].astype(jnp.int32) if side is None else side]
        more = (
            dot_first(table[...], upright_refs[n][...]),
            dot_first(table[:fold_side], corner_refs[n][...]),
            dot_first(table[fold_side:], corner_refs[n][...]),
        )
        if side is not None:
            there = place["below"] if side else place["above"]
            more = [jnp.where(there, m, jnp.zeros_like(m)) for m in more]
        core, ahead, behind = core + more[0], ahead + more[1], behind + more[2]
    edge = ahead + pltpu.roll(behind, MARGIN, 1)
    beside = jnp.where(place["half"] == 0, place["left"], place["right"])
    edge = jnp.where(beside, edge, jnp.zeros_like(edge))
    part = jnp.concatenate([core, edge], axis=1).astype(jnp.bfloat16)
    spec_ref[...] = dot(part[:band], columns_ref[0]) + dot(part[band:], columns_ref[1])


def imaging(
    mine_ref,
    other_ref,
    half_ref,
    field_ref,
    spread_ref,
    across_ref,
    kern_ref,
    share_ref,
    gain_ref,
    send_ref,
    level_ref,
    halves_ref,
    coarse_ref,
    *,
    pad,
):
    conds, kerns, band, _ = kern_ref.shape
    grid = 2 * band
    core = spread_ref.shape[1]
    spec = (mine_ref[...] + other_ref[...]) * (1.0 / pad)
    swapped = pltpu.roll(spec, band, 1)
    first = lax.broadcasted_iota(jnp.int32, spec.shape, 1) < band
    spec_same = jnp.where(first, spec, swapped)
    spec_cross = jnp.where(first, -swapped, spec)

    def condition(c, halves_ref):
        prods = []
        for k in range(kerns):
            kern = kern_ref[c, k].astype(jnp.float32)
            prod = kern * spec_same + pltpu.roll(kern, band, 1) * spec_cross
            prods.append(prod.astype(jnp.bfloat16))
        halves_ref[...] = dot(jnp.concatenate(prods, axis=0), half_ref[...]).astype(jnp.bfloat16)
        total = jnp.zeros((grid, grid), jnp.float32)
        for k in range(0, kerns, 2):
            a = halves_ref[k * band : (k + 1) * band]
            b = halves_ref[(k + 1) * band : (k + 2) * band]
            both = jnp.concatenate(
                [
                    jnp.concatenate([a[:, :grid], b[:, :grid]], axis=1),
                    jnp.concatenate([a[:, grid:], b[:, grid:]], axis=1),
                ],
                axis=0,
            )
            field = dot(field_ref[...], both)
            power = field[:grid] * field[:grid] + field[grid:] * field[grid:]
            shares = share_ref[pl.ds(c * kerns + k, 1)], share_ref[pl.ds(c * kerns + k + 1, 1)]
            total = total + shares[0] * power[:, :grid] + shares[1] * power[:, grid:]
        coarse_ref[c] = total

    turns = 4

    def turn(i, carry):
        for j in range(turns):
            condition(i * turns + j, halves_ref.at[j])
        return carry

    if conds == turns:
        turn(0, 0)
    else:
        lax.fori_loop(0, conds // turns, turn, 0)
    high, low = split(coarse_ref[...].reshape(conds * grid, grid))
    twice = jnp.concatenate([across_ref[0], across_ref[0]], axis=0)
    across = dot(jnp.concatenate([high, low], axis=1), twice) + dot(high, across_ref[1])
    level_ref[0], level_ref[1] = split(across)
    most, least = band_of(1 - lax.axis_index("cond"), level_ref, gain_ref, spread_ref)
    send_ref[0] = most.astype(jnp.bfloat16)
    send_ref[1] = least.astype(jnp.bfloat16)


def band_of(part_of, level_ref, gain_ref, spread_ref):
    conds = gain_ref.shape[1]
    core = spread_ref.shape[1]
    grid = level_ref.shape[1] // conds
    share = core // 2
    rows = pl.ds(pl.multiple_of(part_of * share, share), share)
    fine, rest = spread_ref[0, rows], spread_ref[1, rows]
    twice = jnp.concatenate([fine, fine], axis=1)
    for c in range(conds):
        h = level_ref[0, c * grid : (c + 1) * grid]
        l = level_ref[1, c * grid : (c + 1) * grid]
        blurred = dot(twice, jnp.concatenate([h, l], axis=0)) + dot(rest, h)
        level = gain_ref[0, c, :1] * blurred - gain_ref[1, c, :1]
        most = level if c == 0 else jnp.maximum(most, level)
        least = level if c == 0 else jnp.minimum(least, level)
    return jax.nn.sigmoid(most), jax.nn.sigmoid(least)


def own_share(level_ref, gain_ref, spread_ref, keep_ref):
    keep_ref[0], keep_ref[1] = band_of(lax.axis_index("cond"), level_ref, gain_ref, spread_ref)


def two_parts(table):
    high = np.asarray(table, np.float32).astype(jnp.bfloat16)
    low = (table - high.astype(np.float64)).astype(jnp.bfloat16)
    return np.stack([high, low])


def in_hbm(value):
    return pltpu.with_memory_space_constraint(value, pltpu.HBM)


def shifted(block, axis, distance):
    count = lax.axis_size(axis)
    return lax.ppermute(block, axis, [((i - distance) % count, i) for i in range(count)])


def on_device(mask, kernels, socs_weight, dose, threshold):
    tile = mask[0]
    core = tile.shape[0]
    conds, kerns, band, _ = kernels.shape
    pad = core + 2 * MARGIN
    grid = 2 * band
    place = placement()
    count = lax.axis_size("tile")
    columns, grid_rows = place["columns"], place["grid_rows"]

    half, wide = core // 2, 2 * MARGIN
    sides = (None,) if grid_rows == 2 else (0, 1)
    vmem = pl.BlockSpec(memory_space=pltpu.VMEM)
    hbm = pl.BlockSpec(memory_space=pltpu.HBM)
    params = pltpu.CompilerParams(vmem_limit_bytes=16 * 2**20)
    strip, *blocks = pl.pallas_call(
        lambda *refs: cut(*refs, sides=sides),
        out_shape=[jax.ShapeDtypeStruct((core // 2, wide), tile.dtype)]
        + [jax.ShapeDtypeStruct((MARGIN, half), tile.dtype)] * len(sides)
        + [jax.ShapeDtypeStruct((MARGIN // 2, wide), tile.dtype)] * len(sides),
        in_specs=[hbm],
        out_specs=[vmem] * (1 + 2 * len(sides)),
        scratch_shapes=[
            pltpu.VMEM((core, wide), tile.dtype),
            pltpu.SemaphoreType.DMA((1 + len(sides),)),
        ],
        compiler_params=params,
        name="cut",
    )(in_hbm(tile))

    def passed(block, shift):
        pairs = []
        for t in range(count):
            pairs.append((2 * ((t - shift - 1) % count), 2 * t))
            pairs.append((2 * ((t - shift + 1) % count) + 1, 2 * t + 1))
        return lax.ppermute(block, ("tile", "cond"), pairs)

    shifts = [-columns if side else columns for side in sides]
    strip = passed(strip, 0)
    corners = [passed(t, d) for t, d in zip(blocks[len(sides) :], shifts)]
    uprights = [shifted(t, "tile", d) for t, d in zip(blocks, shifts)]
    row_core, row_side, col_table, half_t, field_t, spread = make_tables(core, band)
    bf = lambda t: jnp.asarray(np.asarray(t).astype(jnp.bfloat16))
    fixed = [
        bf(col_table),
        bf(row_core),
        bf(row_side),
        bf(half_t),
        bf(field_t),
        jnp.asarray(two_parts(spread)),
        jnp.asarray(two_parts(spread.T)),
        kernels,
    ]
    share = core // lax.axis_size("cond")
    outs = [jax.ShapeDtypeStruct(t.shape, t.dtype) for t in fixed]
    outs[0] = jax.ShapeDtypeStruct(fixed[0].shape[1:], fixed[0].dtype)
    outs += [
        jax.ShapeDtypeStruct((core, half), tile.dtype),
        jax.ShapeDtypeStruct((2 * band, half), jnp.float32),
        jax.ShapeDtypeStruct((conds * kerns, grid), jnp.float32),
        jax.ShapeDtypeStruct((2, conds, 8, core), jnp.float32),
    ]
    scalars = (socs_weight, dose, threshold)
    (col_v, row_v, side_v, half_v, field_v, spread_v, across_v, kernels_v, tile_v, part, *gains) = (
        pl.pallas_call(
            lambda *refs: staging(*refs, count=len(fixed)),
            out_shape=outs,
            in_specs=[hbm] * (4 + len(fixed)),
            out_specs=[vmem] * len(outs),
            scratch_shapes=[pltpu.SMEM(t.shape, t.dtype) for t in scalars]
            + [pltpu.SemaphoreType.DMA((4 + len(fixed),))],
            compiler_params=params,
            name="staging",
        )(*map(in_hbm, (tile, *scalars, *fixed)))
    )
    mine = pl.pallas_call(
        lambda *refs: spectrum(*refs, sides=sides),
        out_shape=jax.ShapeDtypeStruct((band, grid), jnp.float32),
        in_specs=[vmem] * (5 + 2 * len(sides)),
        out_specs=vmem,
        compiler_params=params,
        name="spectrum",
    )(part, row_v, side_v, col_v, strip, *uprights, *corners)
    other = lax.ppermute(mine, "cond", [(0, 1), (1, 0)])
    send, level = pl.pallas_call(
        lambda *refs: imaging(*refs, pad=pad),
        out_shape=(
            jax.ShapeDtypeStruct((2, share, core), jnp.bfloat16),
            jax.ShapeDtypeStruct((2, conds * grid, core), jnp.bfloat16),
        ),
        in_specs=[vmem] * 9,
        out_specs=(vmem, vmem),
        scratch_shapes=[
            pltpu.VMEM((4, kerns * band, 2 * grid), jnp.bfloat16),
            pltpu.VMEM((conds, grid, grid), jnp.float32),
        ],
        compiler_params=params,
        name="imaging",
    )(mine, other, half_v, field_v, spread_v, across_v, kernels_v, *gains)
    other = lax.ppermute(send, "cond", [(0, 1), (1, 0)])
    keep = pl.pallas_call(
        own_share,
        out_shape=jax.ShapeDtypeStruct((2, share, core), jnp.float32),
        in_specs=[vmem] * 3,
        out_specs=vmem,
        compiler_params=params,
        name="own_share",
    )(level, gains[1], spread_v)
    other = other.astype(jnp.float32)
    return (jnp.maximum(keep[0], other[0])[None], jnp.minimum(keep[1], other[1])[None])


def solution(mesh):
    return jax.shard_map(
        on_device,
        mesh=mesh,
        in_specs=(
            P(("parts", "tile"), None, None),
            P("cond", None, None, None),
            P("cond", None),
            P("cond"),
            P("cond"),
        ),
        out_specs=(P(("parts", "tile"), "cond", None), P(("parts", "tile"), "cond", None)),
        check_vma=False,
    )
```

```python
import math

import jax
import jax.numpy as jnp
import numpy as np
from jax import lax
from jax.experimental import pallas as pl
from jax.experimental.pallas import tpu as pltpu
from jax.sharding import PartitionSpec as P

MARGIN = 64
BLUR = 8

diffusion = 2.0
steepness = 8.0


def phases(pixels, freqs, period):
    angle = 2.0 * np.pi * ((pixels[:, None] * freqs[None, :]) % period) / period
    return np.cos(angle), np.sin(angle)


def make_tables(core, band):
    pad = core + 2 * MARGIN
    freqs = np.arange(band) - band // 2
    cos_in, sin_in = phases(np.arange(pad), freqs, pad)
    row_all = np.concatenate([cos_in, -sin_in], axis=1).T
    row_core = row_all[:, MARGIN : MARGIN + core]
    row_side = np.stack([row_all[:, :MARGIN].T, row_all[:, MARGIN + core :].T])
    table = np.stack(
        [np.concatenate([cos_in, -sin_in], axis=1), np.concatenate([sin_in, cos_in], axis=1)]
    )
    none = np.zeros((2, MARGIN, 2 * band))
    half = core // 2
    middle = MARGIN + half
    columns = np.stack(
        [
            np.concatenate([table[:, MARGIN:middle], none, table[:, :MARGIN]], axis=1),
            np.concatenate([table[:, middle : middle + half], table[:, -MARGIN:], none], axis=1),
        ]
    )
    grid = 2 * band
    cos_g, sin_g = phases(np.arange(grid), freqs, grid)
    half_table = np.concatenate(
        [np.concatenate([cos_g.T, sin_g.T], axis=1), np.concatenate([-sin_g.T, cos_g.T], axis=1)],
        axis=0,
    )
    field_table = np.concatenate(
        [np.concatenate([cos_g, -sin_g], axis=1), np.concatenate([sin_g, cos_g], axis=1)], axis=0
    )
    pixel = np.arange(core + 2 * BLUR) + MARGIN - BLUR
    sample = np.arange(grid) * (pad / grid)
    degrees = np.arange(1, grid // 2)
    gap = pixel[:, None] - sample[None, :]
    interp = (
        1.0 + 2.0 * np.cos(2.0 * np.pi * gap[:, :, None] * degrees / pad).sum(axis=-1)
    ) / grid
    offset = np.arange(core + 2 * BLUR)[None, :] - np.arange(core)[:, None] - BLUR
    taps = np.where(
        np.abs(offset) <= BLUR, np.exp(-(offset**2) / (2.0 * diffusion * diffusion)), 0.0
    )
    reach = np.arange(-BLUR, BLUR + 1)
    taps = taps / np.exp(-(reach**2) / (2.0 * diffusion * diffusion)).sum()
    spread = taps @ interp
    return row_core, row_side, columns, half_table, field_table, spread


def split(value):
    high = value.astype(jnp.bfloat16)
    low = (value - high.astype(jnp.float32)).astype(jnp.bfloat16)
    return high, low


def dot(a, b):
    return jnp.dot(a, b, preferred_element_type=jnp.float32)


def placement():
    count = lax.axis_size("tile")
    columns = min(8, count // 2)
    grid_rows = count // columns
    position = (lax.axis_index("tile") + columns // 2) % count
    column = position % columns
    row = position // columns
    return dict(
        columns=columns,
        grid_rows=grid_rows,
        right=column < columns - 1,
        left=column > 0,
        above=row > 0,
        below=row < grid_rows - 1,
        top=row == 0,
        side=(lax.axis_index("cond") == column % 2).astype(jnp.int32),
    )


def dot_first(a, b):
    return lax.dot_general(a, b, (((0,), (0,)), ((), ())), preferred_element_type=jnp.float32)


def native_lanes(shape):
    upper = (lax.broadcasted_iota(jnp.int32, shape, 1) >= MARGIN).astype(jnp.int32)
    return upper == placement()["side"]


def folded(block):
    rows = block.shape[0] // 2
    block = block.astype(jnp.float32)
    back = pltpu.roll(block[rows:], MARGIN, 1)
    return jnp.where(native_lanes(back.shape), block[:rows], back).astype(jnp.bfloat16)


def dma_all(pairs, sems):
    return [pltpu.make_async_copy(src, dst, sems.at[n]) for n, (src, dst) in enumerate(pairs)]


def staging(*refs, count):
    tile_hbm, weight_hbm, dose_hbm, threshold_hbm, columns_hbm = refs[:5]
    sources = refs[5 : count + 4]
    columns_ref, *targets = refs[count + 4 : 2 * count + 4]
    tile_ref, part_ref, share_ref, gain_ref, weight_ref, dose_ref, threshold_ref, sems = refs[
        2 * count + 4 :
    ]
    core, half = tile_ref.shape
    own = placement()["side"]
    first = pl.multiple_of(own * half, half)
    pairs = [
        (weight_hbm, weight_ref),
        (dose_hbm, dose_ref),
        (threshold_hbm, threshold_ref),
        (tile_hbm.at[:, pl.ds(first, half)], tile_ref),
        *zip(sources, targets),
        (columns_hbm.at[own], columns_ref),
    ]
    copies = dma_all(pairs, sems)
    for copy in copies:
        copy.start()
    for copy in copies[:5]:
        copy.wait()
    row_core_ref = targets[0]
    part_ref[...] = dot(row_core_ref[...], tile_ref[...])
    conds, kerns = weight_hbm.shape
    scale = float(row_core_ref.shape[0] // 2) ** 2
    for c in range(conds):
        mass = weight_ref[c, 0]
        for k in range(kerns):
            mass = mass + weight_ref[c, k] if k else mass
            share_ref[c * kerns + k, :] = jnp.full((share_ref.shape[1],), weight_ref[c, k])
        gain_ref[0, c] = steepness * dose_ref[c] / jnp.full((8, core), mass * scale)
        gain_ref[1, c] = jnp.full((8, core), steepness * threshold_ref[c])
    for copy in copies[5:]:
        copy.wait()


def cut(tile_hbm, strip_ref, *refs, sides):
    upright_refs, corner_refs = refs[: len(sides)], refs[len(sides) : 2 * len(sides)]
    block_ref, sems = refs[2 * len(sides) :]
    core, wide = block_ref.shape
    half = upright_refs[0].shape[1]
    own = placement()["side"]
    beside = pl.multiple_of(own * (core - wide), wide)
    first = pl.multiple_of(own * half, half)
    rows = []
    for side in sides:
        if side is None:
            lower = placement()["top"].astype(jnp.int32)
            rows.append(pl.ds(pl.multiple_of(lower * (core - MARGIN), MARGIN), MARGIN))
        else:
            rows.append(pl.ds(0 if side else core - MARGIN, MARGIN))
    pairs = [(tile_hbm.at[:, pl.ds(beside, wide)], block_ref)]
    for r, upright_ref in zip(rows, upright_refs):
        pairs.append((tile_hbm.at[r, pl.ds(first, half)], upright_ref))
    copies = dma_all(pairs, sems)
    for copy in copies:
        copy.start()
    copies[0].wait()
    strip_ref[...] = folded(block_ref[...])
    for r, corner_ref in zip(rows, corner_refs):
        corner_ref[...] = folded(block_ref[r])
    for copy in copies[1:]:
        copy.wait()


def spectrum(core_ref, row_core_ref, row_side_ref, columns_ref, strip_ref, *rest, sides):
    upright_refs, corner_refs = rest[: len(sides)], rest[len(sides) : 2 * len(sides)]
    spec_ref = rest[-1]
    place = placement()
    band = spec_ref.shape[0]
    fold = strip_ref.shape[0]
    fold_side = corner_refs[0].shape[0]
    core = core_ref[...]
    ahead = dot(row_core_ref[:, :fold], strip_ref[...])
    behind = dot(row_core_ref[:, fold:], strip_ref[...])
    for n, side in enumerate(sides):
        table = row_side_ref.at[place["top"].astype(jnp.int32) if side is None else side]
        more = (
            dot_first(table[...], upright_refs[n][...]),
            dot_first(table[:fold_side], corner_refs[n][...]),
            dot_first(table[fold_side:], corner_refs[n][...]),
        )
        if side is not None:
            there = place["below"] if side else place["above"]
            more = [jnp.where(there, m, jnp.zeros_like(m)) for m in more]
        core, ahead, behind = core + more[0], ahead + more[1], behind + more[2]
    edge = ahead + pltpu.roll(behind, MARGIN, 1)
    beside = jnp.where(place["side"] == 0, place["left"], place["right"])
    edge = jnp.where(beside, edge, jnp.zeros_like(edge))
    part = jnp.concatenate([core, edge], axis=1).astype(jnp.bfloat16)
    spec_ref[...] = dot(part[:band], columns_ref[0]) + dot(part[band:], columns_ref[1])


def imaging(
    mine_ref,
    other_ref,
    half_ref,
    field_ref,
    spread_ref,
    across_ref,
    kern_ref,
    share_ref,
    gain_ref,
    send_ref,
    level_ref,
    halves_ref,
    coarse_ref,
    *,
    pad,
):
    conds, kerns, band, _ = kern_ref.shape
    grid = 2 * band
    core = spread_ref.shape[1]
    spec = (mine_ref[...] + other_ref[...]) * (1.0 / pad)
    swapped = pltpu.roll(spec, band, 1)
    first = lax.broadcasted_iota(jnp.int32, spec.shape, 1) < band
    spec_same = jnp.where(first, spec, swapped)
    spec_cross = jnp.where(first, -swapped, spec)

    def condition(c, halves_ref):
        prods = []
        for k in range(kerns):
            kern = kern_ref[c, k].astype(jnp.float32)
            prod = kern * spec_same + pltpu.roll(kern, band, 1) * spec_cross
            prods.append(prod.astype(jnp.bfloat16))
        halves_ref[...] = dot(jnp.concatenate(prods, axis=0), half_ref[...]).astype(jnp.bfloat16)
        total = jnp.zeros((grid, grid), jnp.float32)
        for k in range(0, kerns, 2):
            a = halves_ref[k * band : (k + 1) * band]
            b = halves_ref[(k + 1) * band : (k + 2) * band]
            both = jnp.concatenate(
                [
                    jnp.concatenate([a[:, :grid], b[:, :grid]], axis=1),
                    jnp.concatenate([a[:, grid:], b[:, grid:]], axis=1),
                ],
                axis=0,
            )
            field = dot(field_ref[...], both)
            power = field[:grid] * field[:grid] + field[grid:] * field[grid:]
            shares = share_ref[pl.ds(c * kerns + k, 1)], share_ref[pl.ds(c * kerns + k + 1, 1)]
            total = total + shares[0] * power[:, :grid] + shares[1] * power[:, grid:]
        coarse_ref[c] = total

    turns = 4

    def turn(i, carry):
        for j in range(turns):
            condition(i * turns + j, halves_ref.at[j])
        return carry

    if conds == turns:
        turn(0, 0)
    else:
        lax.fori_loop(0, conds // turns, turn, 0)
    high, low = split(coarse_ref[...].reshape(conds * grid, grid))
    twice = jnp.concatenate([across_ref[0], across_ref[0]], axis=0)
    across = dot(jnp.concatenate([high, low], axis=1), twice) + dot(high, across_ref[1])
    level_ref[0], level_ref[1] = split(across)
    most, least = band_of(1 - lax.axis_index("cond"), level_ref, gain_ref, spread_ref)
    send_ref[0] = most.astype(jnp.bfloat16)
    send_ref[1] = least.astype(jnp.bfloat16)


def band_of(part_of, level_ref, gain_ref, spread_ref):
    conds = gain_ref.shape[1]
    core = spread_ref.shape[1]
    grid = level_ref.shape[1] // conds
    share = core // 2
    rows = pl.ds(pl.multiple_of(part_of * share, share), share)
    fine, rest = spread_ref[0, rows], spread_ref[1, rows]
    twice = jnp.concatenate([fine, fine], axis=1)
    for c in range(conds):
        h = level_ref[0, c * grid : (c + 1) * grid]
        l = level_ref[1, c * grid : (c + 1) * grid]
        blurred = dot(twice, jnp.concatenate([h, l], axis=0)) + dot(rest, h)
        level = gain_ref[0, c, :1] * blurred - gain_ref[1, c, :1]
        most = level if c == 0 else jnp.maximum(most, level)
        least = level if c == 0 else jnp.minimum(least, level)
    return jax.nn.sigmoid(most), jax.nn.sigmoid(least)


def own_share(level_ref, gain_ref, spread_ref, keep_ref):
    keep_ref[0], keep_ref[1] = band_of(lax.axis_index("cond"), level_ref, gain_ref, spread_ref)


def two_parts(table):
    high = np.asarray(table, np.float32).astype(jnp.bfloat16)
    low = (table - high.astype(np.float64)).astype(jnp.bfloat16)
    return np.stack([high, low])


def in_hbm(value):
    return pltpu.with_memory_space_constraint(value, pltpu.HBM)


def shifted(block, axis, distance):
    count = lax.axis_size(axis)
    return lax.ppermute(block, axis, [((i - distance) % count, i) for i in range(count)])


def on_device(mask, kernels, socs_weight, dose, threshold):
    tile = mask[0]
    core = tile.shape[0]
    conds, kerns, band, _ = kernels.shape
    pad = core + 2 * MARGIN
    grid = 2 * band
    place = placement()
    count = lax.axis_size("tile")
    columns, grid_rows = place["columns"], place["grid_rows"]
    assert columns % 4 == 0

    half, wide = core // 2, 2 * MARGIN
    sides = (None,) if grid_rows == 2 else (0, 1)
    vmem = pl.BlockSpec(memory_space=pltpu.VMEM)
    hbm = pl.BlockSpec(memory_space=pltpu.HBM)
    params = pltpu.CompilerParams(vmem_limit_bytes=16 * 2**20)
    strip, *blocks = pl.pallas_call(
        lambda *refs: cut(*refs, sides=sides),
        out_shape=[jax.ShapeDtypeStruct((core // 2, wide), tile.dtype)]
        + [jax.ShapeDtypeStruct((MARGIN, half), tile.dtype)] * len(sides)
        + [jax.ShapeDtypeStruct((MARGIN // 2, wide), tile.dtype)] * len(sides),
        in_specs=[hbm],
        out_specs=[vmem] * (1 + 2 * len(sides)),
        scratch_shapes=[
            pltpu.VMEM((core, wide), tile.dtype),
            pltpu.SemaphoreType.DMA((1 + len(sides),)),
        ],
        compiler_params=params,
        name="cut",
    )(in_hbm(tile))

    def passed(block, shift):
        pairs = []
        for t in range(count):
            for c in range(2):
                partner = t + 1 if t % 2 == c else t - 1
                pairs.append((2 * ((partner - shift) % count) + c, 2 * t + c))
        return lax.ppermute(block, ("tile", "cond"), pairs)

    shifts = [-columns if side else columns for side in sides]
    strip = passed(strip, 0)
    corners = [passed(t, d) for t, d in zip(blocks[len(sides) :], shifts)]
    uprights = [shifted(t, "tile", d) for t, d in zip(blocks, shifts)]
    row_core, row_side, col_table, half_t, field_t, spread = make_tables(core, band)
    bf = lambda t: jnp.asarray(np.asarray(t).astype(jnp.bfloat16))
    fixed = [
        bf(col_table),
        bf(row_core),
        bf(row_side),
        bf(half_t),
        bf(field_t),
        jnp.asarray(two_parts(spread)),
        jnp.asarray(two_parts(spread.T)),
        kernels,
    ]
    share = core // lax.axis_size("cond")
    outs = [jax.ShapeDtypeStruct(t.shape, t.dtype) for t in fixed]
    outs[0] = jax.ShapeDtypeStruct(fixed[0].shape[1:], fixed[0].dtype)
    outs += [
        jax.ShapeDtypeStruct((core, half), tile.dtype),
        jax.ShapeDtypeStruct((2 * band, half), jnp.float32),
        jax.ShapeDtypeStruct((conds * kerns, grid), jnp.float32),
        jax.ShapeDtypeStruct((2, conds, 8, core), jnp.float32),
    ]
    scalars = (socs_weight, dose, threshold)
    (col_v, row_v, side_v, half_v, field_v, spread_v, across_v, kernels_v, tile_v, part, *gains) = (
        pl.pallas_call(
            lambda *refs: staging(*refs, count=len(fixed)),
            out_shape=outs,
            in_specs=[hbm] * (4 + len(fixed)),
            out_specs=[vmem] * len(outs),
            scratch_shapes=[pltpu.SMEM(t.shape, t.dtype) for t in scalars]
            + [pltpu.SemaphoreType.DMA((4 + len(fixed),))],
            compiler_params=params,
            name="staging",
        )(*map(in_hbm, (tile, *scalars, *fixed)))
    )
    mine = pl.pallas_call(
        lambda *refs: spectrum(*refs, sides=sides),
        out_shape=jax.ShapeDtypeStruct((band, grid), jnp.float32),
        in_specs=[vmem] * (5 + 2 * len(sides)),
        out_specs=vmem,
        compiler_params=params,
        name="spectrum",
    )(part, row_v, side_v, col_v, strip, *uprights, *corners)
    other = lax.ppermute(mine, "cond", [(0, 1), (1, 0)])
    send, level = pl.pallas_call(
        lambda *refs: imaging(*refs, pad=pad),
        out_shape=(
            jax.ShapeDtypeStruct((2, share, core), jnp.bfloat16),
            jax.ShapeDtypeStruct((2, conds * grid, core), jnp.bfloat16),
        ),
        in_specs=[vmem] * 9,
        out_specs=(vmem, vmem),
        scratch_shapes=[
            pltpu.VMEM((4, kerns * band, 2 * grid), jnp.bfloat16),
            pltpu.VMEM((conds, grid, grid), jnp.float32),
        ],
        compiler_params=params,
        name="imaging",
    )(mine, other, half_v, field_v, spread_v, across_v, kernels_v, *gains)
    other = lax.ppermute(send, "cond", [(0, 1), (1, 0)])
    keep = pl.pallas_call(
        own_share,
        out_shape=jax.ShapeDtypeStruct((2, share, core), jnp.float32),
        in_specs=[vmem] * 3,
        out_specs=vmem,
        compiler_params=params,
        name="own_share",
    )(level, gains[1], spread_v)
    other = other.astype(jnp.float32)
    return (jnp.maximum(keep[0], other[0])[None], jnp.minimum(keep[1], other[1])[None])


def solution(mesh):
    return jax.shard_map(
        on_device,
        mesh=mesh,
        in_specs=(
            P(("parts", "tile"), None, None),
            P("cond", None, None, None),
            P("cond", None),
            P("cond"),
            P("cond"),
        ),
        out_specs=(P(("parts", "tile"), "cond", None), P(("parts", "tile"), "cond", None)),
        check_vma=False,
    )
```

```python
import math

import jax
import jax.numpy as jnp
import numpy as np
from jax import lax
from jax.experimental import pallas as pl
from jax.experimental.pallas import tpu as pltpu
from jax.sharding import PartitionSpec as P

MARGIN = 64
BLUR = 8

diffusion = 2.0
steepness = 8.0


def phases(pixels, freqs, period):
    angle = 2.0 * np.pi * ((pixels[:, None] * freqs[None, :]) % period) / period
    return np.cos(angle), np.sin(angle)


def make_tables(core, band):
    pad = core + 2 * MARGIN
    freqs = np.arange(band) - band // 2
    cos_in, sin_in = phases(np.arange(pad), freqs, pad)
    row_all = np.concatenate([cos_in, -sin_in], axis=1).T
    row_core = row_all[:, MARGIN : MARGIN + core]
    row_side = np.stack([row_all[:, :MARGIN].T, row_all[:, MARGIN + core :].T])
    table = np.stack(
        [np.concatenate([cos_in, -sin_in], axis=1), np.concatenate([sin_in, cos_in], axis=1)]
    )
    none = np.zeros((2, MARGIN, 2 * band))
    half = core // 2
    middle = MARGIN + half
    columns = np.stack(
        [
            np.concatenate([table[:, MARGIN:middle], none, table[:, :MARGIN]], axis=1),
            np.concatenate([table[:, middle : middle + half], table[:, -MARGIN:], none], axis=1),
        ]
    )
    grid = 2 * band
    cos_g, sin_g = phases(np.arange(grid), freqs, grid)
    half_table = np.concatenate(
        [np.concatenate([cos_g.T, sin_g.T], axis=1), np.concatenate([-sin_g.T, cos_g.T], axis=1)],
        axis=0,
    )
    field_table = np.concatenate(
        [np.concatenate([cos_g, -sin_g], axis=1), np.concatenate([sin_g, cos_g], axis=1)], axis=0
    )
    pixel = np.arange(core + 2 * BLUR) + MARGIN - BLUR
    sample = np.arange(grid) * (pad / grid)
    degrees = np.arange(1, grid // 2)
    gap = pixel[:, None] - sample[None, :]
    interp = (
        1.0 + 2.0 * np.cos(2.0 * np.pi * gap[:, :, None] * degrees / pad).sum(axis=-1)
    ) / grid
    offset = np.arange(core + 2 * BLUR)[None, :] - np.arange(core)[:, None] - BLUR
    taps = np.where(
        np.abs(offset) <= BLUR, np.exp(-(offset**2) / (2.0 * diffusion * diffusion)), 0.0
    )
    reach = np.arange(-BLUR, BLUR + 1)
    taps = taps / np.exp(-(reach**2) / (2.0 * diffusion * diffusion)).sum()
    spread = taps @ interp
    return row_core, row_side, columns, half_table, field_table, spread


def split(value):
    high = value.astype(jnp.bfloat16)
    low = (value - high.astype(jnp.float32)).astype(jnp.bfloat16)
    return high, low


def dot(a, b):
    return jnp.dot(a, b, preferred_element_type=jnp.float32)


def placement():
    count = lax.axis_size("tile")
    columns = min(8, count // 2)
    grid_rows = count // columns
    position = (lax.axis_index("tile") + columns // 2) % count
    column = position % columns
    row = position // columns
    return dict(
        columns=columns,
        grid_rows=grid_rows,
        right=column < columns - 1,
        left=column > 0,
        above=row > 0,
        below=row < grid_rows - 1,
        top=row == 0,
        half=lax.axis_index("cond"),
    )


def dot_first(a, b):
    return lax.dot_general(a, b, (((0,), (0,)), ((), ())), preferred_element_type=jnp.float32)


def native_lanes(shape):
    upper = (lax.broadcasted_iota(jnp.int32, shape, 1) >= MARGIN).astype(jnp.int32)
    return upper != lax.axis_index("cond")


def folded(block):
    rows = block.shape[0] // 2
    block = block.astype(jnp.float32)
    back = pltpu.roll(block[rows:], MARGIN, 1)
    return jnp.where(native_lanes(back.shape), block[:rows], back).astype(jnp.bfloat16)


def dma_all(pairs, sems):
    return [pltpu.make_async_copy(src, dst, sems.at[n]) for n, (src, dst) in enumerate(pairs)]


def staging(*refs, count):
    tile_hbm, weight_hbm, dose_hbm, threshold_hbm, columns_hbm = refs[:5]
    sources = refs[5 : count + 4]
    columns_ref, *targets = refs[count + 4 : 2 * count + 4]
    tile_ref, part_ref, share_ref, gain_ref, weight_ref, dose_ref, threshold_ref, sems = refs[
        2 * count + 4 :
    ]
    core, half = tile_ref.shape
    own = lax.axis_index("cond")
    first = pl.multiple_of(own * half, half)
    pairs = [
        (weight_hbm, weight_ref),
        (dose_hbm, dose_ref),
        (threshold_hbm, threshold_ref),
        (tile_hbm.at[:, pl.ds(first, half)], tile_ref),
        *zip(sources, targets),
        (columns_hbm.at[own], columns_ref),
    ]
    copies = dma_all(pairs, sems)
    for copy in copies:
        copy.start()
    for copy in copies[:5]:
        copy.wait()
    row_core_ref = targets[0]
    part_ref[...] = dot(row_core_ref[...], tile_ref[...])
    conds, kerns = weight_hbm.shape
    scale = float(row_core_ref.shape[0] // 2) ** 2
    for c in range(conds):
        mass = weight_ref[c, 0]
        for k in range(kerns):
            mass = mass + weight_ref[c, k] if k else mass
            share_ref[c * kerns + k, :] = jnp.full((share_ref.shape[1],), weight_ref[c, k])
        gain_ref[0, c] = steepness * dose_ref[c] / jnp.full((8, core), mass * scale)
        gain_ref[1, c] = jnp.full((8, core), steepness * threshold_ref[c])
    for copy in copies[5:]:
        copy.wait()


def cut(tile_hbm, strip_ref, *refs, sides):
    upright_refs, corner_refs = refs[: len(sides)], refs[len(sides) : 2 * len(sides)]
    block_ref, sems = refs[2 * len(sides) :]
    core, wide = block_ref.shape
    half = upright_refs[0].shape[1]
    own = lax.axis_index("cond")
    beside = pl.multiple_of((1 - own) * (core - wide), wide)
    first = pl.multiple_of(own * half, half)
    rows = []
    for side in sides:
        if side is None:
            lower = placement()["top"].astype(jnp.int32)
            rows.append(pl.ds(pl.multiple_of(lower * (core - MARGIN), MARGIN), MARGIN))
        else:
            rows.append(pl.ds(0 if side else core - MARGIN, MARGIN))
    pairs = [(tile_hbm.at[:, pl.ds(beside, wide)], block_ref)]
    for r, upright_ref in zip(rows, upright_refs):
        pairs.append((tile_hbm.at[r, pl.ds(first, half)], upright_ref))
    copies = dma_all(pairs, sems)
    for copy in copies:
        copy.start()
    copies[0].wait()
    strip_ref[...] = folded(block_ref[...])
    for r, corner_ref in zip(rows, corner_refs):
        corner_ref[...] = folded(block_ref[r])
    for copy in copies[1:]:
        copy.wait()


def vertical(place, side, row_side_ref):
    if side is None:
        return row_side_ref.at[place["top"].astype(jnp.int32)], None
    return row_side_ref.at[side], place["below"] if side else place["above"]


def kept(there, value):
    return value if there is None else jnp.where(there, value, jnp.zeros_like(value))


def window(core_ref, row_core_ref, row_side_ref, strip_ref, *rest, sides):
    *upright_refs, out_ref, edge_ref = rest
    place = placement()
    fold = strip_ref.shape[0]
    core = core_ref[...]
    for side, upright_ref in zip(sides, upright_refs):
        table, there = vertical(place, side, row_side_ref)
        core = core + kept(there, dot_first(table[...], upright_ref[...]))
    out_ref[...] = core.astype(jnp.bfloat16)
    ahead = dot(row_core_ref[:, :fold], strip_ref[...])
    behind = dot(row_core_ref[:, fold:], strip_ref[...])
    edge_ref[...] = ahead + pltpu.roll(behind, MARGIN, 1)


def spectrum(core_ref, edge_ref, row_side_ref, columns_ref, *rest, sides):
    *corner_refs, spec_ref = rest
    place = placement()
    band = spec_ref.shape[0]
    half = core_ref.shape[1]
    edge = edge_ref[...]
    for side, corner_ref in zip(sides, corner_refs):
        table, there = vertical(place, side, row_side_ref)
        fold = corner_ref.shape[0]
        behind = pltpu.roll(dot_first(table[fold:], corner_ref[...]), MARGIN, 1)
        edge = edge + kept(there, dot_first(table[:fold], corner_ref[...]) + behind)
    beside = jnp.where(place["half"] == 0, place["left"], place["right"])
    edge = kept(beside, edge).astype(jnp.bfloat16)
    core = core_ref[...]
    spec = dot(core[:band], columns_ref[0, :half]) + dot(core[band:], columns_ref[1, :half])
    spec_ref[...] = (
        spec + dot(edge[:band], columns_ref[0, half:]) + dot(edge[band:], columns_ref[1, half:])
    )


def imaging(
    mine_ref,
    other_ref,
    half_ref,
    field_ref,
    spread_ref,
    across_ref,
    kern_ref,
    share_ref,
    gain_ref,
    send_ref,
    level_ref,
    halves_ref,
    coarse_ref,
    *,
    pad,
):
    conds, kerns, band, _ = kern_ref.shape
    grid = 2 * band
    core = spread_ref.shape[1]
    spec = (mine_ref[...] + other_ref[...]) * (1.0 / pad)
    swapped = pltpu.roll(spec, band, 1)
    first = lax.broadcasted_iota(jnp.int32, spec.shape, 1) < band
    spec_same = jnp.where(first, spec, swapped)
    spec_cross = jnp.where(first, -swapped, spec)

    def condition(c, halves_ref):
        prods = []
        for k in range(kerns):
            kern = kern_ref[c, k].astype(jnp.float32)
            prod = kern * spec_same + pltpu.roll(kern, band, 1) * spec_cross
            prods.append(prod.astype(jnp.bfloat16))
        halves_ref[...] = dot(jnp.concatenate(prods, axis=0), half_ref[...]).astype(jnp.bfloat16)
        total = jnp.zeros((grid, grid), jnp.float32)
        for k in range(0, kerns, 2):
            a = halves_ref[k * band : (k + 1) * band]
            b = halves_ref[(k + 1) * band : (k + 2) * band]
            both = jnp.concatenate(
                [
                    jnp.concatenate([a[:, :grid], b[:, :grid]], axis=1),
                    jnp.concatenate([a[:, grid:], b[:, grid:]], axis=1),
                ],
                axis=0,
            )
            field = dot(field_ref[...], both)
            power = field[:grid] * field[:grid] + field[grid:] * field[grid:]
            shares = share_ref[pl.ds(c * kerns + k, 1)], share_ref[pl.ds(c * kerns + k + 1, 1)]
            total = total + shares[0] * power[:, :grid] + shares[1] * power[:, grid:]
        coarse_ref[c] = total

    for c in range(conds):
        condition(c, halves_ref.at[c])
    twice = jnp.concatenate([across_ref[0], across_ref[0]], axis=0)
    for c in range(conds):
        rows = slice(c * grid, (c + 1) * grid)
        high, low = split(coarse_ref[c])
        across = dot(jnp.concatenate([high, low], axis=1), twice) + dot(high, across_ref[1])
        level_ref[0, rows], level_ref[1, rows] = split(across)
    most, least = band_of(1 - lax.axis_index("cond"), level_ref, gain_ref, spread_ref)
    send_ref[0] = most.astype(jnp.bfloat16)
    send_ref[1] = least.astype(jnp.bfloat16)


def band_of(part_of, level_ref, gain_ref, spread_ref):
    conds = gain_ref.shape[1]
    core = spread_ref.shape[1]
    grid = level_ref.shape[1] // conds
    share = core // 2
    rows = pl.ds(pl.multiple_of(part_of * share, share), share)
    fine, rest = spread_ref[0, rows], spread_ref[1, rows]
    twice = jnp.concatenate([fine, fine], axis=1)
    for c in range(conds):
        h = level_ref[0, c * grid : (c + 1) * grid]
        l = level_ref[1, c * grid : (c + 1) * grid]
        blurred = dot(twice, jnp.concatenate([h, l], axis=0)) + dot(rest, h)
        level = gain_ref[0, c, :1] * blurred - gain_ref[1, c, :1]
        most = level if c == 0 else jnp.maximum(most, level)
        least = level if c == 0 else jnp.minimum(least, level)
    return jax.nn.sigmoid(most), jax.nn.sigmoid(least)


def own_share(level_ref, gain_ref, spread_ref, keep_ref):
    keep_ref[0], keep_ref[1] = band_of(lax.axis_index("cond"), level_ref, gain_ref, spread_ref)


def two_parts(table):
    high = np.asarray(table, np.float32).astype(jnp.bfloat16)
    low = (table - high.astype(np.float64)).astype(jnp.bfloat16)
    return np.stack([high, low])


def in_hbm(value):
    return pltpu.with_memory_space_constraint(value, pltpu.HBM)


def shifted(block, axis, distance):
    count = lax.axis_size(axis)
    return lax.ppermute(block, axis, [((i - distance) % count, i) for i in range(count)])


def on_device(mask, kernels, socs_weight, dose, threshold):
    tile = mask[0]
    core = tile.shape[0]
    conds, kerns, band, _ = kernels.shape
    pad = core + 2 * MARGIN
    grid = 2 * band
    place = placement()
    count = lax.axis_size("tile")
    columns, grid_rows = place["columns"], place["grid_rows"]

    half, wide = core // 2, 2 * MARGIN
    sides = (None,) if grid_rows == 2 else (0, 1)
    vmem = pl.BlockSpec(memory_space=pltpu.VMEM)
    hbm = pl.BlockSpec(memory_space=pltpu.HBM)
    params = pltpu.CompilerParams(vmem_limit_bytes=16 * 2**20)
    strip, *blocks = pl.pallas_call(
        lambda *refs: cut(*refs, sides=sides),
        out_shape=[jax.ShapeDtypeStruct((core // 2, wide), tile.dtype)]
        + [jax.ShapeDtypeStruct((MARGIN, half), tile.dtype)] * len(sides)
        + [jax.ShapeDtypeStruct((MARGIN // 2, wide), tile.dtype)] * len(sides),
        in_specs=[hbm],
        out_specs=[vmem] * (1 + 2 * len(sides)),
        scratch_shapes=[
            pltpu.VMEM((core, wide), tile.dtype),
            pltpu.SemaphoreType.DMA((1 + len(sides),)),
        ],
        compiler_params=params,
        name="cut",
    )(in_hbm(tile))

    def passed(block, shift):
        pairs = []
        for t in range(count):
            pairs.append((2 * ((t - shift - 1) % count), 2 * t))
            pairs.append((2 * ((t - shift + 1) % count) + 1, 2 * t + 1))
        return lax.ppermute(block, ("tile", "cond"), pairs)

    shifts = [-columns if side else columns for side in sides]
    strip = passed(strip, 0)
    corners = [passed(t, d) for t, d in zip(blocks[len(sides) :], shifts)]
    uprights = [shifted(t, "tile", d) for t, d in zip(blocks, shifts)]
    row_core, row_side, col_table, half_t, field_t, spread = make_tables(core, band)
    bf = lambda t: jnp.asarray(np.asarray(t).astype(jnp.bfloat16))
    fixed = [
        bf(col_table),
        bf(row_core),
        bf(row_side),
        bf(half_t),
        bf(field_t),
        jnp.asarray(two_parts(spread)),
        jnp.asarray(two_parts(spread.T)),
        kernels,
    ]
    share = core // lax.axis_size("cond")
    outs = [jax.ShapeDtypeStruct(t.shape, t.dtype) for t in fixed]
    outs[0] = jax.ShapeDtypeStruct(fixed[0].shape[1:], fixed[0].dtype)
    outs += [
        jax.ShapeDtypeStruct((core, half), tile.dtype),
        jax.ShapeDtypeStruct((2 * band, half), jnp.float32),
        jax.ShapeDtypeStruct((conds * kerns, grid), jnp.float32),
        jax.ShapeDtypeStruct((2, conds, 8, core), jnp.float32),
    ]
    scalars = (socs_weight, dose, threshold)
    (col_v, row_v, side_v, half_v, field_v, spread_v, across_v, kernels_v, tile_v, part, *gains) = (
        pl.pallas_call(
            lambda *refs: staging(*refs, count=len(fixed)),
            out_shape=outs,
            in_specs=[hbm] * (4 + len(fixed)),
            out_specs=[vmem] * len(outs),
            scratch_shapes=[pltpu.SMEM(t.shape, t.dtype) for t in scalars]
            + [pltpu.SemaphoreType.DMA((4 + len(fixed),))],
            compiler_params=params,
            name="staging",
        )(*map(in_hbm, (tile, *scalars, *fixed)))
    )
    part, edge = pl.pallas_call(
        lambda *refs: window(*refs, sides=sides),
        out_shape=[
            jax.ShapeDtypeStruct((2 * band, half), jnp.bfloat16),
            jax.ShapeDtypeStruct((2 * band, wide), jnp.float32),
        ],
        in_specs=[vmem] * (4 + len(sides)),
        out_specs=[vmem] * 2,
        compiler_params=params,
        name="window",
    )(part, row_v, side_v, strip, *uprights)
    mine = pl.pallas_call(
        lambda *refs: spectrum(*refs, sides=sides),
        out_shape=jax.ShapeDtypeStruct((band, grid), jnp.float32),
        in_specs=[vmem] * (4 + len(sides)),
        out_specs=vmem,
        compiler_params=params,
        name="spectrum",
    )(part, edge, side_v, col_v, *corners)
    other = lax.ppermute(mine, "cond", [(0, 1), (1, 0)])
    send, level = pl.pallas_call(
        lambda *refs: imaging(*refs, pad=pad),
        out_shape=(
            jax.ShapeDtypeStruct((2, share, core), jnp.bfloat16),
            jax.ShapeDtypeStruct((2, conds * grid, core), jnp.bfloat16),
        ),
        in_specs=[vmem] * 9,
        out_specs=(vmem, vmem),
        scratch_shapes=[
            pltpu.VMEM((conds, kerns * band, 2 * grid), jnp.bfloat16),
            pltpu.VMEM((conds, grid, grid), jnp.float32),
        ],
        compiler_params=params,
        name="imaging",
    )(mine, other, half_v, field_v, spread_v, across_v, kernels_v, *gains)
    other = lax.ppermute(send, "cond", [(0, 1), (1, 0)])
    keep = pl.pallas_call(
        own_share,
        out_shape=jax.ShapeDtypeStruct((2, share, core), jnp.float32),
        in_specs=[vmem] * 3,
        out_specs=vmem,
        compiler_params=params,
        name="own_share",
    )(level, gains[1], spread_v)
    other = other.astype(jnp.float32)
    return (jnp.maximum(keep[0], other[0])[None], jnp.minimum(keep[1], other[1])[None])


def solution(mesh):
    return jax.shard_map(
        on_device,
        mesh=mesh,
        in_specs=(
            P(("parts", "tile"), None, None),
            P("cond", None, None, None),
            P("cond", None),
            P("cond"),
            P("cond"),
        ),
        out_specs=(P(("parts", "tile"), "cond", None), P(("parts", "tile"), "cond", None)),
        check_vma=False,
    )
```

```python
import math

import jax
import jax.numpy as jnp
import numpy as np
from jax import lax
from jax.experimental import pallas as pl
from jax.experimental.pallas import tpu as pltpu
from jax.sharding import PartitionSpec as P

MARGIN = 64
BLUR = 8

diffusion = 2.0
steepness = 8.0


def phases(pixels, freqs, period):
    angle = 2.0 * np.pi * ((pixels[:, None] * freqs[None, :]) % period) / period
    return np.cos(angle), np.sin(angle)


def make_tables(core, band):
    pad = core + 2 * MARGIN
    freqs = np.arange(band) - band // 2
    cos_in, sin_in = phases(np.arange(pad), freqs, pad)
    row_all = np.concatenate([cos_in, -sin_in], axis=1).T
    row_core = row_all[:, MARGIN : MARGIN + core]
    row_side = np.stack([row_all[:, :MARGIN].T, row_all[:, MARGIN + core :].T])
    table = np.stack(
        [np.concatenate([cos_in, -sin_in], axis=1), np.concatenate([sin_in, cos_in], axis=1)]
    )
    none = np.zeros((2, MARGIN, 2 * band))
    half = core // 2
    middle = MARGIN + half
    columns = np.stack(
        [
            np.concatenate([table[:, MARGIN:middle], none, table[:, :MARGIN]], axis=1),
            np.concatenate([table[:, middle : middle + half], table[:, -MARGIN:], none], axis=1),
        ]
    )
    grid = 2 * band
    cos_g, sin_g = phases(np.arange(grid), freqs, grid)
    half_table = np.concatenate(
        [np.concatenate([cos_g.T, sin_g.T], axis=1), np.concatenate([-sin_g.T, cos_g.T], axis=1)],
        axis=0,
    )
    field_table = np.concatenate(
        [np.concatenate([cos_g, -sin_g], axis=1), np.concatenate([sin_g, cos_g], axis=1)], axis=0
    )
    pixel = np.arange(core + 2 * BLUR) + MARGIN - BLUR
    sample = np.arange(grid) * (pad / grid)
    degrees = np.arange(1, grid // 2)
    gap = pixel[:, None] - sample[None, :]
    interp = (
        1.0 + 2.0 * np.cos(2.0 * np.pi * gap[:, :, None] * degrees / pad).sum(axis=-1)
    ) / grid
    offset = np.arange(core + 2 * BLUR)[None, :] - np.arange(core)[:, None] - BLUR
    taps = np.where(
        np.abs(offset) <= BLUR, np.exp(-(offset**2) / (2.0 * diffusion * diffusion)), 0.0
    )
    reach = np.arange(-BLUR, BLUR + 1)
    taps = taps / np.exp(-(reach**2) / (2.0 * diffusion * diffusion)).sum()
    spread = taps @ interp
    return row_core, row_side, columns, half_table, field_table, spread


def split(value):
    high = value.astype(jnp.bfloat16)
    low = (value - high.astype(jnp.float32)).astype(jnp.bfloat16)
    return high, low


def dot(a, b):
    return jnp.dot(a, b, preferred_element_type=jnp.float32)


def placement():
    count = lax.axis_size("tile")
    columns = min(8, count // 2)
    grid_rows = count // columns
    position = (lax.axis_index("tile") + columns // 2) % count
    column = position % columns
    row = position // columns
    return dict(
        columns=columns,
        grid_rows=grid_rows,
        right=column < columns - 1,
        left=column > 0,
        above=row > 0,
        below=row < grid_rows - 1,
        top=row == 0,
        half=lax.axis_index("cond"),
    )


def dot_first(a, b):
    return lax.dot_general(a, b, (((0,), (0,)), ((), ())), preferred_element_type=jnp.float32)


def dma_all(pairs, sems):
    return [pltpu.make_async_copy(src, dst, sems.at[n]) for n, (src, dst) in enumerate(pairs)]


def staging(*refs, count):
    tile_hbm, weight_hbm, dose_hbm, threshold_hbm, columns_hbm = refs[:5]
    sources = refs[5 : count + 4]
    columns_ref, *targets = refs[count + 4 : 2 * count + 4]
    tile_ref, part_ref, share_ref, gain_ref, weight_ref, dose_ref, threshold_ref, sems = refs[
        2 * count + 4 :
    ]
    core, half = tile_ref.shape
    own = lax.axis_index("cond")
    first = pl.multiple_of(own * half, half)
    pairs = [
        (weight_hbm, weight_ref),
        (dose_hbm, dose_ref),
        (threshold_hbm, threshold_ref),
        (tile_hbm.at[:, pl.ds(first, half)], tile_ref),
        *zip(sources, targets),
        (columns_hbm.at[own], columns_ref),
    ]
    copies = dma_all(pairs, sems)
    for copy in copies:
        copy.start()
    for copy in copies[:5]:
        copy.wait()
    row_core_ref = targets[0]
    part_ref[...] = dot(row_core_ref[...], tile_ref[...])
    conds, kerns = weight_hbm.shape
    scale = float(row_core_ref.shape[0] // 2) ** 2
    for c in range(conds):
        mass = weight_ref[c, 0]
        for k in range(kerns):
            mass = mass + weight_ref[c, k] if k else mass
            share_ref[c * kerns + k, :] = jnp.full((share_ref.shape[1],), weight_ref[c, k])
        gain_ref[0, c] = steepness * dose_ref[c] / jnp.full((8, core), mass * scale)
        gain_ref[1, c] = jnp.full((8, core), steepness * threshold_ref[c])
    for copy in copies[5:]:
        copy.wait()


def late_staging(order_ref, *refs):
    count = (len(refs) - 1) // 2
    copies = dma_all(zip(refs[:count], refs[count : 2 * count]), refs[-1])
    for copy in copies:
        copy.start()
    for copy in copies:
        copy.wait()


def cut(tile_hbm, strip_ref, *refs, sides):
    upright_refs, corner_refs = refs[: len(sides)], refs[len(sides) : 2 * len(sides)]
    sems = refs[-1]
    core, wide = strip_ref.shape
    half = upright_refs[0].shape[1]
    own = lax.axis_index("cond")
    beside = pl.multiple_of((1 - own) * (core - wide), wide)
    first = pl.multiple_of(own * half, half)
    rows = []
    for side in sides:
        if side is None:
            lower = placement()["top"].astype(jnp.int32)
            rows.append(pl.ds(pl.multiple_of(lower * (core - MARGIN), MARGIN), MARGIN))
        else:
            rows.append(pl.ds(0 if side else core - MARGIN, MARGIN))
    pairs = [(tile_hbm.at[:, pl.ds(beside, wide)], strip_ref)]
    for r, upright_ref, corner_ref in zip(rows, upright_refs, corner_refs):
        pairs.append((tile_hbm.at[r, pl.ds(first, half)], upright_ref))
        pairs.append((tile_hbm.at[r, pl.ds(beside, wide)], corner_ref))
    copies = dma_all(pairs, sems)
    for copy in copies:
        copy.start()
    for copy in copies:
        copy.wait()


def vertical(place, side, row_side_ref):
    if side is None:
        return row_side_ref.at[place["top"].astype(jnp.int32)], None
    return row_side_ref.at[side], place["below"] if side else place["above"]


def kept(there, value):
    return value if there is None else jnp.where(there, value, jnp.zeros_like(value))


def window(core_ref, row_core_ref, row_side_ref, strip_ref, *rest, sides):
    *upright_refs, out_ref, edge_ref = rest
    place = placement()
    core = core_ref[...]
    for side, upright_ref in zip(sides, upright_refs):
        table, there = vertical(place, side, row_side_ref)
        core = core + kept(there, dot_first(table[...], upright_ref[...]))
    out_ref[...] = core.astype(jnp.bfloat16)
    edge_ref[...] = dot(row_core_ref[...], strip_ref[...])


def spectrum(core_ref, edge_ref, row_side_ref, columns_ref, *rest, sides):
    *corner_refs, spec_ref = rest
    place = placement()
    band = spec_ref.shape[0]
    half = core_ref.shape[1]
    edge = edge_ref[...]
    for side, corner_ref in zip(sides, corner_refs):
        table, there = vertical(place, side, row_side_ref)
        edge = edge + kept(there, dot_first(table[...], corner_ref[...]))
    beside = jnp.where(place["half"] == 0, place["left"], place["right"])
    edge = kept(beside, edge).astype(jnp.bfloat16)
    core = core_ref[...]
    spec = dot(core[:band], columns_ref[0, :half]) + dot(core[band:], columns_ref[1, :half])
    spec_ref[...] = (
        spec + dot(edge[:band], columns_ref[0, half:]) + dot(edge[band:], columns_ref[1, half:])
    )


def imaging(
    mine_ref,
    other_ref,
    half_ref,
    field_ref,
    spread_ref,
    across_ref,
    kern_ref,
    share_ref,
    gain_ref,
    send_ref,
    level_ref,
    halves_ref,
    coarse_ref,
    *,
    pad,
):
    conds, kerns, band, _ = kern_ref.shape
    grid = 2 * band
    core = spread_ref.shape[1]
    spec = (mine_ref[...] + other_ref[...]) * (1.0 / pad)
    swapped = pltpu.roll(spec, band, 1)
    first = lax.broadcasted_iota(jnp.int32, spec.shape, 1) < band
    spec_same = jnp.where(first, spec, swapped)
    spec_cross = jnp.where(first, -swapped, spec)

    def condition(c, halves_ref):
        for k in range(0, kerns, 12):
            prods = []
            for m in range(k, k + 12):
                kern = kern_ref[c, m].astype(jnp.float32)
                prod = kern * spec_same + pltpu.roll(kern, band, 1) * spec_cross
                prods.append(prod.astype(jnp.bfloat16))
            half = dot(jnp.concatenate(prods, axis=0), half_ref[...]).astype(jnp.bfloat16)
            halves_ref[k * band : (k + 12) * band] = half
        total = jnp.zeros((grid, grid), jnp.float32)
        for k in range(0, kerns, 2):
            a = halves_ref[k * band : (k + 1) * band]
            b = halves_ref[(k + 1) * band : (k + 2) * band]
            both = jnp.concatenate(
                [
                    jnp.concatenate([a[:, :grid], b[:, :grid]], axis=1),
                    jnp.concatenate([a[:, grid:], b[:, grid:]], axis=1),
                ],
                axis=0,
            )
            field = dot(field_ref[...], both)
            power = field[:grid] * field[:grid] + field[grid:] * field[grid:]
            shares = share_ref[pl.ds(c * kerns + k, 1)], share_ref[pl.ds(c * kerns + k + 1, 1)]
            total = total + shares[0] * power[:, :grid] + shares[1] * power[:, grid:]
        coarse_ref[c] = total

    for c in range(conds):
        condition(c, halves_ref.at[c])
    twice = jnp.concatenate([across_ref[0], across_ref[0]], axis=0)
    for c in range(conds):
        rows = slice(c * grid, (c + 1) * grid)
        high, low = split(coarse_ref[c])
        across = dot(jnp.concatenate([high, low], axis=1), twice) + dot(high, across_ref[1])
        level_ref[0, rows], level_ref[1, rows] = split(across)
    most, least = band_of(1 - lax.axis_index("cond"), level_ref, gain_ref, spread_ref)
    send_ref[0] = most.astype(jnp.bfloat16)
    send_ref[1] = least.astype(jnp.bfloat16)


def band_of(part_of, level_ref, gain_ref, spread_ref):
    conds = gain_ref.shape[1]
    core = spread_ref.shape[1]
    grid = level_ref.shape[1] // conds
    share = core // 2
    rows = pl.ds(pl.multiple_of(part_of * share, share), share)
    fine, rest = spread_ref[0, rows], spread_ref[1, rows]
    twice = jnp.concatenate([fine, fine], axis=1)
    for c in range(conds):
        h = level_ref[0, c * grid : (c + 1) * grid]
        l = level_ref[1, c * grid : (c + 1) * grid]
        blurred = dot(twice, jnp.concatenate([h, l], axis=0)) + dot(rest, h)
        level = gain_ref[0, c, :1] * blurred - gain_ref[1, c, :1]
        most = level if c == 0 else jnp.maximum(most, level)
        least = level if c == 0 else jnp.minimum(least, level)
    return jax.nn.sigmoid(most), jax.nn.sigmoid(least)


def own_share(level_ref, gain_ref, spread_ref, keep_ref):
    keep_ref[0], keep_ref[1] = band_of(lax.axis_index("cond"), level_ref, gain_ref, spread_ref)


def two_parts(table):
    high = np.asarray(table, np.float32).astype(jnp.bfloat16)
    low = (table - high.astype(np.float64)).astype(jnp.bfloat16)
    return np.stack([high, low])


def in_hbm(value):
    return pltpu.with_memory_space_constraint(value, pltpu.HBM)


def shifted(block, axis, distance):
    count = lax.axis_size(axis)
    return lax.ppermute(block, axis, [((i - distance) % count, i) for i in range(count)])


def on_device(mask, kernels, socs_weight, dose, threshold):
    tile = mask[0]
    core = tile.shape[0]
    conds, kerns, band, _ = kernels.shape
    pad = core + 2 * MARGIN
    grid = 2 * band
    place = placement()
    count = lax.axis_size("tile")
    columns, grid_rows = place["columns"], place["grid_rows"]

    half, wide = core // 2, 2 * MARGIN
    sides = (None,) if grid_rows == 2 else (0, 1)
    vmem = pl.BlockSpec(memory_space=pltpu.VMEM)
    hbm = pl.BlockSpec(memory_space=pltpu.HBM)
    params = pltpu.CompilerParams(vmem_limit_bytes=16 * 2**20)
    strip, *blocks = pl.pallas_call(
        lambda *refs: cut(*refs, sides=sides),
        out_shape=[jax.ShapeDtypeStruct((core, wide), tile.dtype)]
        + [jax.ShapeDtypeStruct((MARGIN, half), tile.dtype)] * len(sides)
        + [jax.ShapeDtypeStruct((MARGIN, wide), tile.dtype)] * len(sides),
        in_specs=[hbm],
        out_specs=[vmem] * (1 + 2 * len(sides)),
        scratch_shapes=[
            pltpu.SemaphoreType.DMA((1 + 2 * len(sides),)),
        ],
        compiler_params=params,
        name="cut",
    )(in_hbm(tile))

    def passed(block, shift):
        pairs = []
        for t in range(count):
            pairs.append((2 * ((t - shift - 1) % count), 2 * t))
            pairs.append((2 * ((t - shift + 1) % count) + 1, 2 * t + 1))
        return lax.ppermute(block, ("tile", "cond"), pairs)

    shifts = [-columns if side else columns for side in sides]
    strip = passed(strip, 0)
    corners = [passed(t, d) for t, d in zip(blocks[len(sides) :], shifts)]
    uprights = [shifted(t, "tile", d) for t, d in zip(blocks, shifts)]
    row_core, row_side, col_table, half_t, field_t, spread = make_tables(core, band)
    bf = lambda t: jnp.asarray(np.asarray(t).astype(jnp.bfloat16))
    fixed = [
        bf(col_table),
        bf(row_core),
        bf(row_side),
        bf(half_t),
        bf(field_t),
        kernels,
    ]
    fixed_late = [jnp.asarray(two_parts(spread)), jnp.asarray(two_parts(spread.T))]
    share = core // lax.axis_size("cond")
    outs = [jax.ShapeDtypeStruct(t.shape, t.dtype) for t in fixed]
    outs[0] = jax.ShapeDtypeStruct(fixed[0].shape[1:], fixed[0].dtype)
    outs += [
        jax.ShapeDtypeStruct((core, half), tile.dtype),
        jax.ShapeDtypeStruct((2 * band, half), jnp.float32),
        jax.ShapeDtypeStruct((conds * kerns, grid), jnp.float32),
        jax.ShapeDtypeStruct((2, conds, 8, core), jnp.float32),
    ]
    scalars = (socs_weight, dose, threshold)
    (col_v, row_v, side_v, half_v, field_v, kernels_v, tile_v, part, *gains) = (
        pl.pallas_call(
            lambda *refs: staging(*refs, count=len(fixed)),
            out_shape=outs,
            in_specs=[hbm] * (4 + len(fixed)),
            out_specs=[vmem] * len(outs),
            scratch_shapes=[pltpu.SMEM(t.shape, t.dtype) for t in scalars]
            + [pltpu.SemaphoreType.DMA((4 + len(fixed),))],
            compiler_params=params,
            name="staging",
        )(*map(in_hbm, (tile, *scalars, *fixed)))
    )
    part, edge = pl.pallas_call(
        lambda *refs: window(*refs, sides=sides),
        out_shape=[
            jax.ShapeDtypeStruct((2 * band, half), jnp.bfloat16),
            jax.ShapeDtypeStruct((2 * band, wide), jnp.float32),
        ],
        in_specs=[vmem] * (4 + len(sides)),
        out_specs=[vmem] * 2,
        compiler_params=params,
        name="window",
    )(part, row_v, side_v, strip, *uprights)
    mine = pl.pallas_call(
        lambda *refs: spectrum(*refs, sides=sides),
        out_shape=jax.ShapeDtypeStruct((band, grid), jnp.float32),
        in_specs=[vmem] * (4 + len(sides)),
        out_specs=vmem,
        compiler_params=params,
        name="spectrum",
    )(part, edge, side_v, col_v, *corners)
    other = lax.ppermute(mine, "cond", [(0, 1), (1, 0)])
    late = [fixed_late[0], fixed_late[1]]
    spread_v, across_v = pl.pallas_call(
        late_staging,
        out_shape=[jax.ShapeDtypeStruct(t.shape, t.dtype) for t in late],
        in_specs=[vmem] + [hbm] * len(late),
        out_specs=[vmem] * len(late),
        scratch_shapes=[pltpu.SemaphoreType.DMA((len(late),))],
        compiler_params=params,
        name="late_staging",
    )(mine, *map(in_hbm, late))
    send, level = pl.pallas_call(
        lambda *refs: imaging(*refs, pad=pad),
        out_shape=(
            jax.ShapeDtypeStruct((2, share, core), jnp.bfloat16),
            jax.ShapeDtypeStruct((2, conds * grid, core), jnp.bfloat16),
        ),
        in_specs=[vmem] * 9,
        out_specs=(vmem, vmem),
        scratch_shapes=[
            pltpu.VMEM((conds, kerns * band, 2 * grid), jnp.bfloat16),
            pltpu.VMEM((conds, grid, grid), jnp.float32),
        ],
        compiler_params=params,
        name="imaging",
    )(mine, other, half_v, field_v, spread_v, across_v, kernels_v, *gains)
    other = lax.ppermute(send, "cond", [(0, 1), (1, 0)])
    keep = pl.pallas_call(
        own_share,
        out_shape=jax.ShapeDtypeStruct((2, share, core), jnp.float32),
        in_specs=[vmem] * 3,
        out_specs=vmem,
        compiler_params=params,
        name="own_share",
    )(level, gains[1], spread_v)
    other = other.astype(jnp.float32)
    return (jnp.maximum(keep[0], other[0])[None], jnp.minimum(keep[1], other[1])[None])


def solution(mesh):
    return jax.shard_map(
        on_device,
        mesh=mesh,
        in_specs=(
            P(("parts", "tile"), None, None),
            P("cond", None, None, None),
            P("cond", None),
            P("cond"),
            P("cond"),
        ),
        out_specs=(P(("parts", "tile"), "cond", None), P(("parts", "tile"), "cond", None)),
        check_vma=False,
    )
```
